256 devices in a mesh: data: 256 (over z, y, x, core).
Axes of the slice: x: 4, y: 4, z: 8, core: 2. Of those that a mesh axis runs over, the one named last changes fastest.
Arguments:
- z_one: bfloat16 [16384, 256], P('data')
- z_two: bfloat16 [16384, 256], P('data')
- protos: bfloat16 [8192, 256], replicated
- queue_one: bfloat16 [131072, 256], P('data')
- queue_two: bfloat16 [131072, 256], P('data')
Outputs:
- output 1: float32 [16384, 8192], P('data')
- output 2: float32 [16384, 8192], P('data')
- output 3: float32 [], replicated
- output 4: float32 [16384, 256], P('data')
- output 5: float32 [16384, 256], P('data')
- output 6: float32 [8192, 256], replicated
All inputs are finite; a program needn't handle non-finite values.
Results may differ from the reference program's by a relative error of at most 0.001.
Values are sent between devices in bfloat16 or wider.
A program may use at most 768 MiB of HBM per device.

```python
import jax
import jax.numpy as jnp
from jax import lax

PROTOS = 8192
EMBED_DIM = 256
GROUP_SIZE = 256
ROWS_DEV = 64
QUEUE_DEV = 512
SINKHORN_ITERS = 3
EPSILON = 0.05
TEMPERATURE = 0.1


def unit_rows(values):
    return values / jnp.sqrt(jnp.sum(values * values, axis=-1, keepdims=True))


def setup_inputs(seed: int = 0) -> dict:
    key_list = jax.random.split(jax.random.key(seed), 8)
    noise_scale = EMBED_DIM ** -0.5
    batch_shape = (GROUP_SIZE, ROWS_DEV, EMBED_DIM)
    queue_shape = (GROUP_SIZE, QUEUE_DEV, EMBED_DIM)
    centers = unit_rows(jax.random.normal(key_list[0], (GROUP_SIZE, 1, EMBED_DIM), jnp.float32))
    queue_centers = unit_rows(jax.random.normal(key_list[1], (GROUP_SIZE, 1, EMBED_DIM), jnp.float32))
    base_rows = 1.5 * centers + noise_scale * jax.random.normal(key_list[2], batch_shape, jnp.float32)
    view_one = unit_rows(base_rows + 0.5 * noise_scale * jax.random.normal(key_list[3], batch_shape, jnp.float32))
    view_two = unit_rows(base_rows + 0.5 * noise_scale * jax.random.normal(key_list[4], batch_shape, jnp.float32))
    queue_one = unit_rows(1.5 * queue_centers + noise_scale * jax.random.normal(key_list[5], queue_shape, jnp.float32))
    queue_two = unit_rows(1.5 * queue_centers + noise_scale * jax.random.normal(key_list[6], queue_shape, jnp.float32))
    protos = unit_rows(jax.random.normal(key_list[7], (PROTOS, EMBED_DIM), jnp.float32))
    return {
        "z_one": view_one.reshape(GROUP_SIZE * ROWS_DEV, EMBED_DIM).astype(jnp.bfloat16),
        "z_two": view_two.reshape(GROUP_SIZE * ROWS_DEV, EMBED_DIM).astype(jnp.bfloat16),
        "protos": protos.astype(jnp.bfloat16),
        "queue_one": queue_one.reshape(GROUP_SIZE * QUEUE_DEV, EMBED_DIM).astype(jnp.bfloat16),
        "queue_two": queue_two.reshape(GROUP_SIZE * QUEUE_DEV, EMBED_DIM).astype(jnp.bfloat16),
    }


def scores_of(row_block, protos):
    return jnp.dot(row_block, protos.T, preferred_element_type=jnp.float32)


def scaled_col_sum(blocks, protos, col_scale, total_rows):
    def pass_body(col_acc, row_block):
        transport = jnp.exp(scores_of(row_block, protos) / EPSILON)
        row_scale = 1.0 / (total_rows * jnp.sum(transport * col_scale, axis=1))
        return col_acc + jnp.sum(transport * row_scale[:, None], axis=0), None
    col_sum, _ = lax.scan(pass_body, jnp.zeros((PROTOS,), jnp.float32), blocks)
    return col_sum


def column_scale(blocks, protos):
    total_rows = GROUP_SIZE * (ROWS_DEV + QUEUE_DEV)

    def first_body(col_acc, row_block):
        transport = jnp.exp(scores_of(row_block, protos) / EPSILON)
        return col_acc + jnp.sum(transport, axis=0), None

    col_sum, _ = lax.scan(first_body, jnp.zeros((PROTOS,), jnp.float32), blocks)
    col_scale = 1.0 / (PROTOS * col_sum)
    for _ in range(SINKHORN_ITERS - 1):
        col_scale = 1.0 / (PROTOS * scaled_col_sum(blocks, protos, col_scale, total_rows))
    return col_scale


def reference(z_one, z_two, protos, queue_one, queue_two):
    batch_one = z_one.reshape(GROUP_SIZE, ROWS_DEV, EMBED_DIM)
    batch_two = z_two.reshape(GROUP_SIZE, ROWS_DEV, EMBED_DIM)
    rows_all_one = jnp.concatenate([batch_one, queue_one.reshape(GROUP_SIZE, QUEUE_DEV, EMBED_DIM)], axis=1)
    rows_all_two = jnp.concatenate([batch_two, queue_two.reshape(GROUP_SIZE, QUEUE_DEV, EMBED_DIM)], axis=1)
    scale_one = column_scale(rows_all_one, protos)
    scale_two = column_scale(rows_all_two, protos)
    batch_total = GROUP_SIZE * ROWS_DEV
    grad_coef = 1.0 / (2 * batch_total * TEMPERATURE)

    def block_step(carry, row_blocks):
        loss_acc, proto_acc = carry
        rows_one, rows_two = row_blocks
        score_one = scores_of(rows_one, protos)
        score_two = scores_of(rows_two, protos)
        plan_one = jnp.exp(score_one / EPSILON) * scale_one
        plan_two = jnp.exp(score_two / EPSILON) * scale_two
        codes_one = plan_one / jnp.sum(plan_one, axis=1, keepdims=True)
        codes_two = plan_two / jnp.sum(plan_two, axis=1, keepdims=True)
        logp_one = jax.nn.log_softmax(score_one / TEMPERATURE, axis=1)
        logp_two = jax.nn.log_softmax(score_two / TEMPERATURE, axis=1)
        part_loss = jnp.sum(codes_two * logp_one) + jnp.sum(codes_one * logp_two)
        grad_s_one = ((jnp.exp(logp_one) - codes_two) * grad_coef).astype(jnp.bfloat16)
        grad_s_two = ((jnp.exp(logp_two) - codes_one) * grad_coef).astype(jnp.bfloat16)
        dz_one = jnp.dot(grad_s_one, protos, preferred_element_type=jnp.float32)
        dz_two = jnp.dot(grad_s_two, protos, preferred_element_type=jnp.float32)
        proto_part = jnp.dot(grad_s_one.T, rows_one, preferred_element_type=jnp.float32) + jnp.dot(grad_s_two.T, rows_two, preferred_element_type=jnp.float32)
        return (loss_acc + part_loss, proto_acc + proto_part), (codes_one, codes_two, dz_one, dz_two)

    start_carry = (jnp.zeros((), jnp.float32), jnp.zeros((PROTOS, EMBED_DIM), jnp.float32))
    (loss_sum, grad_protos), (codes_one, codes_two, dz_one, dz_two) = lax.scan(block_step, start_carry, (batch_one, batch_two))
    swap_loss = -loss_sum / (2 * batch_total)
    return (
        codes_one.reshape(batch_total, PROTOS),
        codes_two.reshape(batch_total, PROTOS),
        swap_loss,
        dz_one.reshape(batch_total, EMBED_DIM),
        dz_two.reshape(batch_total, EMBED_DIM),
        grad_protos,
    )
```

```python
import functools

import jax
import jax.numpy as jnp
from jax import lax
from jax.experimental import pallas as pl
from jax.experimental.pallas import tpu as pltpu
from jax.sharding import PartitionSpec as P

EPSILON = 0.05
TEMPERATURE = 0.1
ITERS = 3
CORES = 2
CHIPS_Z = 8
VMEM_LIMIT = 67043328
ROW_BLOCK = 192
LANES = 128
LOG2E = 1.4426950408889634
F32 = jnp.float32
MESH = pl.DeviceIdType.MESH


def dot_nt(a, b):
    return lax.dot_general(a, b, (((1,), (1,)), ((), ())), preferred_element_type=F32)


def sinkhorn_kernel(
    nz, plane, total_rows, protos_count,
    z_one, z_two, q_one, q_two, protos,
    scale_out,
    rows, cols, mat, wacc, rscale, csum, rs_buf, ex_buf, ag_buf,
    row_sem, col_sem, out_sem, rs_send, rs_recv, ex_send, ex_recv, ag_send, ag_recv,
):
    me = lax.axis_index("data")
    core = lax.rem(me, CORES)
    chip = lax.div(me, CORES)
    yx = lax.rem(chip, plane)
    zz = lax.div(chip, plane)
    members = nz * CORES
    mine = zz * CORES + core
    tiles = mat.shape[1]
    per = tiles // members
    n_rows = mat.shape[2]
    batch = z_one.shape[0]
    wide = per * LANES
    blocks = n_rows // ROW_BLOCK if n_rows % ROW_BLOCK == 0 else 1
    rb = n_rows // blocks

    def near(t):
        k, e = lax.div(t, 2), lax.rem(t, 2)
        j = lax.div(k + 1, 2)
        dz = j * (2 * lax.rem(k, 2) - 1)
        return lax.rem(zz + dz + nz, nz) * CORES + lax.rem(core + e, CORES)

    def member_dev(m):
        return (lax.div(m, CORES) * plane + yx) * CORES + lax.rem(m, CORES)

    def plane_dev(o):
        return (zz * plane + o) * CORES + core

    views = ((z_one, q_one), (z_two, q_two))
    row_copies = []
    for v, (z, q) in enumerate(views):
        row_copies.append([
            pltpu.make_async_copy(z, rows.at[v, pl.ds(0, batch)], row_sem.at[v, 0]),
            pltpu.make_async_copy(q, rows.at[v, pl.ds(batch, n_rows - batch)], row_sem.at[v, 1]),
        ])

    def col_copy(m):
        part = pl.ds(pl.multiple_of(m * wide, wide), wide)
        return pltpu.make_async_copy(protos.at[part], cols.at[part], col_sem.at[m])

    for c in row_copies[0]:
        c.start()

    def start_cols(t, carry):
        col_copy(near(members - 1 - t)).start()
        return carry

    lax.fori_loop(0, members, start_cols, 0)
    for c in row_copies[1]:
        c.start()

    barrier = pltpu.get_barrier_semaphore()

    def greet_members(t, carry):
        pl.semaphore_signal(barrier, inc=1, device_id=(member_dev(near(t)),), device_id_type=MESH)
        return carry

    def greet_plane(t, carry):
        pl.semaphore_signal(barrier, inc=1, device_id=(plane_dev(lax.rem(yx + t, plane)),), device_id_type=MESH)
        return carry

    lax.fori_loop(1, members, greet_members, 0)
    lax.fori_loop(1, plane, greet_plane, 0)

    def rs_copy(it, v, m):
        return pltpu.make_async_remote_copy(
            src_ref=csum.at[it, v, m], dst_ref=rs_buf.at[it, v, mine],
            send_sem=rs_send.at[it, v], recv_sem=rs_recv.at[it, v],
            device_id=(member_dev(m),), device_id_type=MESH)

    def rs_start(it, v, t):
        rs_copy(it, v, near(members - 1 - t)).start()

    def rs_start_all(it, v):
        def send(t, carry):
            rs_start(it, v, t)
            return carry
        lax.fori_loop(0, members - 1, send, 0)

    def first_pass(v):
        for c in row_copies[v]:
            c.wait()

        def step(t, carry):
            m = near(members - 1 - t)
            if v == 0:
                col_copy(m).wait()
            part = pl.ds(pl.multiple_of(m * wide, wide), wide)
            scores = dot_nt(rows[v], cols[part, :])
            for j in range(per):
                e = jnp.exp2(scores[:, j * LANES:(j + 1) * LANES] * (LOG2E / EPSILON))
                mat[v, m * per + j] = e
                csum[0, v, m, pl.ds(j, 1), :] = jnp.sum(e, axis=0, keepdims=True)
            return carry

        lax.fori_loop(0, members, step, 0)

    first_pass(0)
    pl.semaphore_wait(barrier, members + plane - 2)
    rs_start_all(0, 0)
    first_pass(1)
    rs_start_all(0, 1)

    def wait_bytes(ref, sem):
        pltpu.make_async_copy(ref, ref, sem).wait()

    def reduce_slice(it, v):
        wait_bytes(rs_buf.at[it, v, pl.ds(0, members - 1)], rs_recv.at[it, v])
        rs_buf[it, v, mine] = csum[it, v, mine]
        ex_buf[it, v, yx] = jnp.sum(rs_buf[it, v], axis=0)

        def send(t, carry):
            o = lax.rem(yx + t, plane)
            pltpu.make_async_remote_copy(
                src_ref=ex_buf.at[it, v, yx], dst_ref=ex_buf.at[it, v, yx],
                send_sem=ex_send.at[it, v], recv_sem=ex_recv.at[it, v],
                device_id=(plane_dev(o),), device_id_type=MESH).start()
            return carry

        lax.fori_loop(1, plane, send, 0)

    def share_scale(it, v):
        wait_bytes(ex_buf.at[it, v, pl.ds(0, plane - 1)], ex_recv.at[it, v])
        ag_buf[it, v, mine] = 1.0 / (protos_count * jnp.sum(ex_buf[it, v], axis=0))

        def send(t, carry):
            m = near(members - t)
            pltpu.make_async_remote_copy(
                src_ref=ag_buf.at[it, v, mine], dst_ref=ag_buf.at[it, v, mine],
                send_sem=ag_send.at[it, v], recv_sem=ag_recv.at[it, v, mine],
                device_id=(member_dev(m),), device_id_type=MESH).start()
            return carry

        lax.fori_loop(1, members, send, 0)

    def all_reduce(it):
        for v in range(2):
            reduce_slice(it, v)
        for v in range(2):
            share_scale(it, v)

    def wait_scale(it, v, m):
        wait_bytes(ag_buf.at[it, v, m], ag_recv.at[it, v, m])

    def next_pass(it, v):
        wacc[...] = jnp.zeros_like(wacc)

        def add_slice(t, carry):
            m = near(t)

            @pl.when(t > 0)
            def _():
                wait_scale(it, v, m)

            for b in range(blocks):
                part = pl.ds(b * rb, rb)
                acc = wacc[part, :]
                for j in range(per):
                    acc += mat[v, m * per + j, part, :] * ag_buf[it, v, m, pl.ds(j, 1), :]
                wacc[part, :] = acc
            return carry

        lax.fori_loop(0, members, add_slice, 0)
        row_sum = jnp.sum(wacc[...], axis=1, keepdims=True)
        rscale[...] = jnp.broadcast_to(1.0 / (total_rows * row_sum), rscale.shape)

        def col_slice(t, carry):
            m = near(members - 1 - t)
            acc = [None] * per
            for b in range(blocks):
                part = pl.ds(b * rb, rb)
                r = rscale[part, :]
                for j in range(per):
                    p = (mat[v, m * per + j, part, :] * r).reshape(rb // 8, 8, LANES).sum(axis=0)
                    acc[j] = p if acc[j] is None else acc[j] + p
            for j in range(per):
                csum[it + 1, v, m, pl.ds(j, 1), :] = jnp.sum(acc[j], axis=0, keepdims=True)

            @pl.when(t > 0)
            def _():
                rs_start(it + 1, v, t - 1)
            return carry

        lax.fori_loop(0, members, col_slice, 0)

    def iteration(it, carry):
        all_reduce(it)
        for v in range(2):
            next_pass(it, v)
        return carry

    lax.fori_loop(0, ITERS - 1, iteration, 0)
    last = ITERS - 1
    all_reduce(last)
    outs = []
    for v in range(2):
        def wait_one(t, carry):
            wait_scale(last, v, near(t))
            return carry
        lax.fori_loop(1, members, wait_one, 0)
        outs.append(pltpu.make_async_copy(ag_buf.at[last, v], scale_out.at[v], out_sem.at[v]))
        outs[v].start()

    def drain(it, carry):
        for v in range(2):
            wait_bytes(rs_buf.at[it, v, pl.ds(0, members - 1)], rs_send.at[it, v])
            wait_bytes(ex_buf.at[it, v, pl.ds(0, plane - 1)], ex_send.at[it, v])
            wait_bytes(rs_buf.at[it, v, pl.ds(0, members - 1)], ag_send.at[it, v])
        return carry

    lax.fori_loop(0, ITERS, drain, 0)
    for c in outs:
        c.wait()


def column_scales(nz, plane, z_one, z_two, q_one, q_two, protos):
    batch, dim = z_one.shape
    n_rows = batch + q_one.shape[0]
    count = protos.shape[0]
    tiles = count // LANES
    members = nz * CORES
    per = tiles // members
    total_rows = nz * plane * CORES * n_rows
    any_spec = pl.BlockSpec(memory_space=pl.ANY)
    small = (per, LANES)
    dma = pltpu.SemaphoreType.DMA
    scales = pl.pallas_call(
        functools.partial(sinkhorn_kernel, nz, plane, float(total_rows), float(count)),
        out_shape=jax.ShapeDtypeStruct((2, members) + small, F32),
        in_specs=[any_spec] * 5,
        out_specs=any_spec,
        scratch_shapes=[
            pltpu.VMEM((2, n_rows, dim), jnp.bfloat16),
            pltpu.VMEM((count, dim), jnp.bfloat16),
            pltpu.VMEM((2, tiles, n_rows, LANES), F32),
            pltpu.VMEM((n_rows, LANES), F32),
            pltpu.VMEM((n_rows, LANES), F32),
            pltpu.VMEM((ITERS, 2, members) + small, F32),
            pltpu.VMEM((ITERS, 2, members) + small, F32),
            pltpu.VMEM((ITERS, 2, plane) + small, F32),
            pltpu.VMEM((ITERS, 2, members) + small, F32),
            dma((2, 2)),
            dma((members,)),
            dma((2,)),
            dma((ITERS, 2)),
            dma((ITERS, 2)),
            dma((ITERS, 2)),
            dma((ITERS, 2)),
            dma((ITERS, 2)),
            dma((ITERS, 2, members)),
        ],
        compiler_params=pltpu.CompilerParams(
            collective_id=0, has_side_effects=True, vmem_limit_bytes=VMEM_LIMIT),
        name="sinkhorn",
    )(z_one, z_two, q_one, q_two, protos)
    return scales.reshape(2, count)


def solution(mesh, nz=CHIPS_Z):
    group_size = mesh.shape["data"]
    plane = group_size // (nz * CORES)

    def local_step(z_one, z_two, protos, queue_one, queue_two):
        batch_rows = z_one.shape[0]
        batch_total = group_size * batch_rows
        scales = column_scales(nz, plane, z_one, z_two, queue_one, queue_two, protos)

        def codes_of(z, scale):
            score = dot_nt(z, protos)
            plan = jnp.exp(score / EPSILON) * scale
            return plan / jnp.sum(plan, axis=1, keepdims=True), score

        codes_one, score_one = codes_of(z_one, scales[0])
        codes_two, score_two = codes_of(z_two, scales[1])
        logp_one = jax.nn.log_softmax(score_one / TEMPERATURE, axis=1)
        logp_two = jax.nn.log_softmax(score_two / TEMPERATURE, axis=1)
        part_loss = jnp.sum(codes_two * logp_one) + jnp.sum(codes_one * logp_two)
        swap_loss = -lax.psum(part_loss, "data") / (2 * batch_total)
        grad_coef = 1.0 / (2 * batch_total * TEMPERATURE)
        grad_s_one = ((jnp.exp(logp_one) - codes_two) * grad_coef).astype(jnp.bfloat16)
        grad_s_two = ((jnp.exp(logp_two) - codes_one) * grad_coef).astype(jnp.bfloat16)
        dz_one = jnp.dot(grad_s_one, protos, preferred_element_type=F32)
        dz_two = jnp.dot(grad_s_two, protos, preferred_element_type=F32)
        proto_part = (jnp.einsum("nk,nd->kd", grad_s_one, z_one, preferred_element_type=F32)
                      + jnp.einsum("nk,nd->kd", grad_s_two, z_two, preferred_element_type=F32))
        grad_protos = lax.psum(proto_part, "data")
        return codes_one, codes_two, swap_loss, dz_one, dz_two, grad_protos

    row_spec = P("data", None)
    full_spec = P(None, None)
    return jax.shard_map(
        local_step,
        mesh=mesh,
        in_specs=(row_spec, row_spec, full_spec, row_spec, row_spec),
        out_specs=(row_spec, row_spec, P(), row_spec, row_spec, full_spec),
        check_vma=False,
    )
```

```python
import functools

import jax
import jax.numpy as jnp
from jax import lax
from jax.experimental import pallas as pl
from jax.experimental.pallas import tpu as pltpu
from jax.sharding import PartitionSpec as P

EPSILON = 0.05
TEMPERATURE = 0.1
ITERS = 3
CORES = 2
CHIPS_Z = 8
CHIPS_X = 4
VMEM_LIMIT = 67043328
ROW_BLOCK = 192
LANES = 128
LOG2E = 1.4426950408889634
F32 = jnp.float32
MESH = pl.DeviceIdType.MESH


def dot_nt(a, b):
    return lax.dot_general(a, b, (((1,), (1,)), ((), ())), preferred_element_type=F32)


def sinkhorn_kernel(
    nz, plane, total_rows, protos_count,
    z_one, z_two, q_one, q_two, protos,
    scale_out,
    rows, cols, mat, wacc, rscale, csum, rs_buf, ex_buf, ag_buf,
    row_sem, col_sem, out_sem, rs_send, rs_recv, ex_send, ex_recv, ag_send, ag_recv,
):
    me = lax.axis_index("data")
    core = lax.rem(me, CORES)
    chip = lax.div(me, CORES)
    yx = lax.rem(chip, plane)
    zz = lax.div(chip, plane)
    members = nz * CORES
    mine = zz * CORES + core
    tiles = mat.shape[1]
    per = tiles // members
    n_rows = mat.shape[2]
    batch = z_one.shape[0]
    wide = per * LANES
    blocks = n_rows // ROW_BLOCK if n_rows % ROW_BLOCK == 0 else 1
    rb = n_rows // blocks

    def near(t):
        k, e = lax.div(t, 2), lax.rem(t, 2)
        j = lax.div(k + 1, 2)
        dz = j * (2 * lax.rem(k, 2) - 1)
        return lax.rem(zz + dz + nz, nz) * CORES + lax.rem(core + e, CORES)

    def member_dev(m):
        return (lax.div(m, CORES) * plane + yx) * CORES + lax.rem(m, CORES)

    def plane_dev(o):
        return (zz * plane + o) * CORES + core

    views = ((z_one, q_one), (z_two, q_two))
    row_copies = []
    for v, (z, q) in enumerate(views):
        row_copies.append([
            pltpu.make_async_copy(z, rows.at[v, pl.ds(0, batch)], row_sem.at[v, 0]),
            pltpu.make_async_copy(q, rows.at[v, pl.ds(batch, n_rows - batch)], row_sem.at[v, 1]),
        ])

    def col_copy(m):
        part = pl.ds(pl.multiple_of(m * wide, wide), wide)
        return pltpu.make_async_copy(protos.at[part], cols.at[part], col_sem.at[m])

    for c in row_copies[0]:
        c.start()

    def start_cols(t, carry):
        col_copy(near(members - 1 - t)).start()
        return carry

    lax.fori_loop(0, members, start_cols, 0)
    for c in row_copies[1]:
        c.start()

    barrier = pltpu.get_barrier_semaphore()

    def greet_members(t, carry):
        pl.semaphore_signal(barrier, inc=1, device_id=(member_dev(near(t)),), device_id_type=MESH)
        return carry

    def greet_plane(t, carry):
        pl.semaphore_signal(barrier, inc=1, device_id=(plane_dev(lax.rem(yx + t, plane)),), device_id_type=MESH)
        return carry

    lax.fori_loop(1, members, greet_members, 0)
    lax.fori_loop(1, plane, greet_plane, 0)

    def rs_copy(it, v, m):
        return pltpu.make_async_remote_copy(
            src_ref=csum.at[it, v, m], dst_ref=rs_buf.at[it, v, mine],
            send_sem=rs_send.at[it, v], recv_sem=rs_recv.at[it, v],
            device_id=(member_dev(m),), device_id_type=MESH)

    def rs_start(it, v, t):
        rs_copy(it, v, near(members - 1 - t)).start()

    def rs_start_all(it, v):
        def send(t, carry):
            rs_start(it, v, t)
            return carry
        lax.fori_loop(0, members - 1, send, 0)

    def first_pass(v):
        for c in row_copies[v]:
            c.wait()

        def step(t, carry):
            m = near(members - 1 - t)
            if v == 0:
                col_copy(m).wait()
            part = pl.ds(pl.multiple_of(m * wide, wide), wide)
            scores = dot_nt(rows[v], cols[part, :])
            for j in range(per):
                e = jnp.exp2(scores[:, j * LANES:(j + 1) * LANES] * (LOG2E / EPSILON))
                mat[v, m * per + j] = e
                csum[0, v, m, pl.ds(j, 1), :] = jnp.sum(e, axis=0, keepdims=True)
            return carry

        lax.fori_loop(0, members, step, 0)

    first_pass(0)
    pl.semaphore_wait(barrier, members + plane - 2)
    rs_start_all(0, 0)
    first_pass(1)
    rs_start_all(0, 1)

    def wait_bytes(ref, sem):
        pltpu.make_async_copy(ref, ref, sem).wait()

    def reduce_slice(it, v):
        wait_bytes(rs_buf.at[it, v, pl.ds(0, members - 1)], rs_recv.at[it, v])
        rs_buf[it, v, mine] = csum[it, v, mine]
        ex_buf[it, v, yx] = jnp.sum(rs_buf[it, v], axis=0)

        def send(t, carry):
            o = lax.rem(yx + t, plane)
            pltpu.make_async_remote_copy(
                src_ref=ex_buf.at[it, v, yx], dst_ref=ex_buf.at[it, v, yx],
                send_sem=ex_send.at[it, v], recv_sem=ex_recv.at[it, v],
                device_id=(plane_dev(o),), device_id_type=MESH).start()
            return carry

        lax.fori_loop(1, plane, send, 0)

    def share_scale(it, v):
        wait_bytes(ex_buf.at[it, v, pl.ds(0, plane - 1)], ex_recv.at[it, v])
        ag_buf[it, v, mine] = 1.0 / (protos_count * jnp.sum(ex_buf[it, v], axis=0))

        def send(t, carry):
            m = near(members - t)
            pltpu.make_async_remote_copy(
                src_ref=ag_buf.at[it, v, mine], dst_ref=ag_buf.at[it, v, mine],
                send_sem=ag_send.at[it, v], recv_sem=ag_recv.at[it, v, mine],
                device_id=(member_dev(m),), device_id_type=MESH).start()
            return carry

        lax.fori_loop(1, members, send, 0)

    def all_reduce(it):
        for v in range(2):
            reduce_slice(it, v)
        for v in range(2):
            share_scale(it, v)

    def wait_scale(it, v, m):
        wait_bytes(ag_buf.at[it, v, m], ag_recv.at[it, v, m])

    def next_pass(it, v):
        wacc[...] = jnp.zeros_like(wacc)

        def add_slice(t, carry):
            m = near(t)

            @pl.when(t > 0)
            def _():
                wait_scale(it, v, m)

            for b in range(blocks):
                part = pl.ds(b * rb, rb)
                acc = wacc[part, :]
                for j in range(per):
                    acc += mat[v, m * per + j, part, :] * ag_buf[it, v, m, pl.ds(j, 1), :]
                wacc[part, :] = acc
            return carry

        lax.fori_loop(0, members, add_slice, 0)
        row_sum = jnp.sum(wacc[...], axis=1, keepdims=True)
        rscale[...] = jnp.broadcast_to(1.0 / (total_rows * row_sum), rscale.shape)

        def col_slice(t, carry):
            m = near(members - 1 - t)
            acc = [None] * per
            for b in range(blocks):
                part = pl.ds(b * rb, rb)
                r = rscale[part, :]
                for j in range(per):
                    p = (mat[v, m * per + j, part, :] * r).reshape(rb // 8, 8, LANES).sum(axis=0)
                    acc[j] = p if acc[j] is None else acc[j] + p
            for j in range(per):
                csum[it + 1, v, m, pl.ds(j, 1), :] = jnp.sum(acc[j], axis=0, keepdims=True)

            @pl.when(t > 0)
            def _():
                rs_start(it + 1, v, t - 1)
            return carry

        lax.fori_loop(0, members, col_slice, 0)

    def iteration(it, carry):
        all_reduce(it)
        for v in range(2):
            next_pass(it, v)
        return carry

    lax.fori_loop(0, ITERS - 1, iteration, 0)
    last = ITERS - 1
    all_reduce(last)
    outs = []
    for v in range(2):
        def wait_one(t, carry):
            wait_scale(last, v, near(t))
            return carry
        lax.fori_loop(1, members, wait_one, 0)
        outs.append(pltpu.make_async_copy(ag_buf.at[last, v], scale_out.at[v], out_sem.at[v]))
        outs[v].start()

    def drain(it, carry):
        for v in range(2):
            wait_bytes(rs_buf.at[it, v, pl.ds(0, members - 1)], rs_send.at[it, v])
            wait_bytes(ex_buf.at[it, v, pl.ds(0, plane - 1)], ex_send.at[it, v])
            wait_bytes(rs_buf.at[it, v, pl.ds(0, members - 1)], ag_send.at[it, v])
        return carry

    lax.fori_loop(0, ITERS, drain, 0)
    for c in outs:
        c.wait()


def column_scales(nz, plane, z_one, z_two, q_one, q_two, protos):
    batch, dim = z_one.shape
    n_rows = batch + q_one.shape[0]
    count = protos.shape[0]
    tiles = count // LANES
    members = nz * CORES
    per = tiles // members
    total_rows = nz * plane * CORES * n_rows
    any_spec = pl.BlockSpec(memory_space=pl.ANY)
    small = (per, LANES)
    dma = pltpu.SemaphoreType.DMA
    scales = pl.pallas_call(
        functools.partial(sinkhorn_kernel, nz, plane, float(total_rows), float(count)),
        out_shape=jax.ShapeDtypeStruct((2, members) + small, F32),
        in_specs=[any_spec] * 5,
        out_specs=any_spec,
        scratch_shapes=[
            pltpu.VMEM((2, n_rows, dim), jnp.bfloat16),
            pltpu.VMEM((count, dim), jnp.bfloat16),
            pltpu.VMEM((2, tiles, n_rows, LANES), F32),
            pltpu.VMEM((n_rows, LANES), F32),
            pltpu.VMEM((n_rows, LANES), F32),
            pltpu.VMEM((ITERS, 2, members) + small, F32),
            pltpu.VMEM((ITERS, 2, members) + small, F32),
            pltpu.VMEM((ITERS, 2, plane) + small, F32),
            pltpu.VMEM((ITERS, 2, members) + small, F32),
            dma((2, 2)),
            dma((members,)),
            dma((2,)),
            dma((ITERS, 2)),
            dma((ITERS, 2)),
            dma((ITERS, 2)),
            dma((ITERS, 2)),
            dma((ITERS, 2)),
            dma((ITERS, 2, members)),
        ],
        compiler_params=pltpu.CompilerParams(
            collective_id=0, has_side_effects=True, vmem_limit_bytes=VMEM_LIMIT),
        name="sinkhorn",
    )(z_one, z_two, q_one, q_two, protos)
    return scales.reshape(2, count)


def codes_kernel(
    grad_coef, z_one, z_two, protos, scale_refs,
    codes_one, codes_two, grad_out, dz_one, dz_two, loss_out,
    cols, score, plan, prob, col_sem, out_sem,
):
    chunks, batch, wide = score.shape[1:]
    rows = (z_one, z_two)
    scales = scale_refs

    def col_copy(t):
        part = pl.ds(pl.multiple_of(t * wide, wide), wide)
        return pltpu.make_async_copy(protos.at[part], cols.at[part], col_sem.at[t])

    def start(t, carry):
        col_copy(t).start()
        return carry

    lax.fori_loop(0, chunks, start, 0)
    zero = jnp.zeros((batch, LANES), F32)
    per = wide // LANES

    def lane_fold(x):
        return sum(x[:, j * LANES:(j + 1) * LANES] for j in range(per))

    def scan(t, carry):
        col_copy(t).wait()
        part = pl.ds(pl.multiple_of(t * wide, wide), wide)
        sums = []
        for v in range(2):
            s = dot_nt(rows[v][...], cols[part, :])
            score[v, t] = s
            b = jnp.exp2(s * (LOG2E / TEMPERATURE))
            prob[v, t] = b
            a = jnp.exp2(s * (LOG2E / EPSILON)) * scales[v, pl.ds(t, 1), :]
            plan[v, t] = a
            sums += [carry[2 * v] + lane_fold(a), carry[2 * v + 1] + lane_fold(b)]
        return tuple(sums)

    sums = lax.fori_loop(0, chunks, scan, (zero,) * 4)
    row_sum = [jnp.sum(x, axis=1, keepdims=True) for x in sums]
    inv = [1.0 / x for x in row_sum]
    lse = [jnp.log(row_sum[2 * v + 1]) for v in range(2)]

    def code_copy(v, t):
        out = (codes_one, codes_two)[v]
        return pltpu.make_async_copy(
            plan.at[v, t], out.at[:, pl.ds(pl.multiple_of(t * wide, wide), wide)], out_sem.at[v])

    def finish(t, carry):
        loss, dz = carry
        part = pl.ds(pl.multiple_of(t * wide, wide), wide)
        codes = [plan[v, t] * inv[2 * v] for v in range(2)]
        for v in range(2):
            plan[v, t] = codes[v]
        grads = []
        for v in range(2):
            p = prob[v, t] * inv[2 * v + 1]
            other = codes[1 - v]
            grads.append(((p - other) * grad_coef).astype(jnp.bfloat16))
            loss = loss + lane_fold(other * (score[v, t] * (1.0 / TEMPERATURE) - lse[v]))
        both = jnp.concatenate(grads, axis=0)
        grad_out[t] = both
        dz = dz + jnp.dot(both, cols[part, :], preferred_element_type=F32)
        for v in range(2):
            code_copy(v, t).start()
        return loss, dz

    loss, dz = lax.fori_loop(
        0, chunks, finish, (zero, jnp.zeros((2 * batch, cols.shape[1]), F32)))
    dz_one[...] = dz[:batch]
    dz_two[...] = dz[batch:]
    loss_out[...] = jnp.sum(loss, axis=0, keepdims=True)

    def drain(t, carry):
        for v in range(2):
            code_copy(v, t).wait()
        return carry

    lax.fori_loop(0, chunks, drain, 0)


def batch_codes(chunks, grad_coef, z_one, z_two, protos, scales):
    batch, dim = z_one.shape
    count = protos.shape[0]
    wide = count // chunks
    any_spec = pl.BlockSpec(memory_space=pl.ANY)
    vmem = pl.BlockSpec(memory_space=pltpu.VMEM)
    big = pltpu.VMEM((2, chunks, batch, wide), F32)
    return pl.pallas_call(
        functools.partial(codes_kernel, grad_coef),
        out_shape=(
            jax.ShapeDtypeStruct((batch, count), F32),
            jax.ShapeDtypeStruct((batch, count), F32),
            jax.ShapeDtypeStruct((chunks, 2 * batch, wide), jnp.bfloat16),
            jax.ShapeDtypeStruct((batch, dim), F32),
            jax.ShapeDtypeStruct((batch, dim), F32),
            jax.ShapeDtypeStruct((1, LANES), F32),
        ),
        in_specs=[vmem, vmem, any_spec, vmem],
        out_specs=(any_spec, any_spec, vmem, vmem, vmem, vmem),
        scratch_shapes=[
            pltpu.VMEM((count, dim), jnp.bfloat16), big, big, big,
            pltpu.SemaphoreType.DMA((chunks,)), pltpu.SemaphoreType.DMA((2,)),
        ],
        compiler_params=pltpu.CompilerParams(vmem_limit_bytes=48 * 2 ** 20),
        name="codes",
    )(z_one, z_two, protos, scales.reshape(2, chunks, wide))


def protos_kernel(
    nz, ny, nx,
    grads, z_rows, loss_in,
    total, loss_out,
    g_buf, z_buf, part_buf, y_buf, yz_buf, sums, loss_buf,
    own_sem, z_send, z_recv, g_send, g_recv, p_send, p_recv, s_send, s_recv,
    az_send, az_recv, ay_send, ay_recv, ax_send, ax_recv, af_send, af_recv, pair_send, pair_recv,
    out_sem, l_send, l_recv,
):
    me = lax.axis_index("data")
    core = lax.rem(me, CORES)
    chip = lax.div(me, CORES)
    x = lax.rem(chip, nx)
    y = lax.rem(lax.div(chip, nx), ny)
    z = lax.div(chip, nx * ny)
    halves = 2

    def dev(xx, yy, z2, cc):
        return ((z2 * ny + yy) * nx + xx) * CORES + cc

    def remote(src, dst, send, recv, device):
        return pltpu.make_async_remote_copy(
            src_ref=src, dst_ref=dst, send_sem=send, recv_sem=recv, device_id=(device,), device_id_type=MESH)

    def wait_bytes(ref, sem):
        pltpu.make_async_copy(ref, ref, sem).wait()

    n_first, n_second = (nx, ny), (ny, nx)
    first, second = (x, y), (y, x)

    def dev_first(col, f, cc):
        return dev(f, y, z, cc) if col == 0 else dev(x, f, z, cc)

    def dev_second(col, s):
        return dev(x, s, z, core) if col == 0 else dev(s, y, z, core)

    members = [n_first[col] * CORES for col in range(2)]
    slot = [first[col] * CORES + core for col in range(2)]

    def member_dev(col, m):
        return dev_first(col, lax.div(m, CORES), lax.rem(m, CORES))

    barrier = pltpu.get_barrier_semaphore()
    greeted = 0
    for col in range(2):
        for t in range(1, members[col]):
            if col == 1 and t == 1:
                continue
            f = lax.rem(first[col] + t // CORES, n_first[col])
            cc = lax.rem(core + t % CORES, CORES)
            pl.semaphore_signal(barrier, inc=1, device_id=(dev_first(col, f, cc),), device_id_type=MESH)
            greeted += 1
    for t in range(1, nz):
        pl.semaphore_signal(barrier, inc=1, device_id=(dev(x, y, lax.rem(z + t, nz), core),), device_id_type=MESH)
        greeted += 1

    own_z = pltpu.make_async_copy(z_rows, z_buf.at[0, slot[0]], own_sem.at[0])
    own_z2 = pltpu.make_async_copy(z_rows, z_buf.at[1, slot[1]], own_sem.at[1])
    own_l = pltpu.make_async_copy(loss_in, loss_buf.at[0, slot[0]], own_sem.at[2])
    own_z.start()
    own_z2.start()
    own_l.start()
    own_z.wait()
    own_z2.wait()
    own_l.wait()
    pl.semaphore_wait(barrier, greeted)

    width = part_buf.shape[2]
    order = [(h, col) for h in range(halves) for col in range(2)]

    def far(n, t):
        offs = sorted(range(1, n), key=lambda d: -min(d, n - d))
        return offs[t]

    def group_offsets(col):
        n = n_first[col]
        offs = [(far(n, t), c) for t in range(n - 1) for c in range(CORES)]
        return offs + [(0, 1)]

    for col in range(2):
        for df, dc in group_offsets(col):
            f = lax.rem(first[col] + df, n_first[col])
            cc = lax.rem(core + dc, CORES)
            remote(z_buf.at[col, slot[col]], z_buf.at[col, slot[col]],
                   z_send.at[col], z_recv.at[col], dev_first(col, f, cc)).start()
    for h, col in order:
        for df, dc in group_offsets(col):
            f = lax.rem(first[col] + df, n_first[col])
            cc = lax.rem(core + dc, CORES)
            m = f * CORES + cc
            block = (col * members[col] + m) * halves + h
            remote(grads.at[block], g_buf.at[col, h, slot[col]],
                   g_send.at[col, h], g_recv.at[col, h], dev_first(col, f, cc)).start()
    for df, dc in group_offsets(0):
        f = lax.rem(first[0] + df, n_first[0])
        cc = lax.rem(core + dc, CORES)
        remote(loss_buf.at[0, slot[0]], loss_buf.at[0, slot[0]], l_send.at[0], l_recv.at[0], dev_first(0, f, cc)).start()

    own_copies = {}
    for n, (h, col) in enumerate(order):
        block = (col * members[col] + slot[col]) * halves + h
        own_copies[h, col] = pltpu.make_async_copy(grads.at[block], g_buf.at[col, h, slot[col]], own_sem.at[3 + n])
        own_copies[h, col].start()

    block_rows = [width // n_second[col] for col in range(2)]
    unit = block_rows[0] // nz

    def address(col, h, f, cc, s, zi):
        half_count = total.shape[0] // 2
        return col * half_count + ((f * CORES + cc) * halves + h) * width + s * block_rows[col] + zi * unit

    def stage_g(h, col):
        own_copies[h, col].wait()
        wait_bytes(g_buf.at[col, h, pl.ds(0, members[col] - 1)], g_recv.at[col, h])
        if h == 0:
            wait_bytes(z_buf.at[col, pl.ds(0, members[col] - 1)], z_recv.at[col])
        k = members[col] * z_buf.shape[2]
        g = g_buf[col, h].reshape(k, width)
        zs = z_buf[col].reshape(k, z_buf.shape[3])
        part_buf[col, h] = lax.dot_general(g, zs, (((0,), (0,)), ((), ())), preferred_element_type=F32)
        for t in range(n_second[col] - 1):
            s = lax.rem(second[col] + far(n_second[col], t), n_second[col])
            rows = pl.ds(pl.multiple_of(s * block_rows[col], 8), block_rows[col])
            remote(part_buf.at[col, h, rows], y_buf.at[col, h, second[col]],
                   p_send.at[col, h], p_recv.at[col, h], dev_second(col, s)).start()

    def stage_y(h, col):
        n = n_second[col]
        wait_bytes(y_buf.at[col, h, pl.ds(0, n - 1)], p_recv.at[col, h])
        mine = pl.ds(pl.multiple_of(second[col] * block_rows[col], 8), block_rows[col])
        y_buf[col, h, second[col]] = part_buf[col, h, mine]
        yz_buf[col, h, 0] = jnp.sum(y_buf[col, h], axis=0)
        for t in range(nz - 1):
            z2 = lax.rem(z + far(nz, t), nz)
            rows = pl.ds(pl.multiple_of(z2 * unit, 8), unit)
            remote(yz_buf.at[col, h, 0, rows], sums.at[col, h, z],
                   s_send.at[col, h], s_recv.at[col, h], dev(x, y, z2, core)).start()

    def rows_of(addr, n):
        return pl.ds(pl.multiple_of(addr, 8), n)

    def stage_z(h, col):
        wait_bytes(sums.at[col, h, pl.ds(0, nz - 1)], s_recv.at[col, h])
        sums[col, h, z] = yz_buf[col, h, 0, pl.ds(pl.multiple_of(z * unit, 8), unit)]
        own = rows_of(address(col, h, first[col], core, second[col], z), unit)
        total[own, :] = jnp.sum(sums[col, h], axis=0)
        for t in range(nz - 1):
            z2 = lax.rem(z + far(nz, t), nz)
            remote(total.at[own], total.at[own], az_send.at[col, h], az_recv.at[col, h], dev(x, y, z2, core)).start()

    def stage_az(h, col):
        n = n_second[col]
        block = rows_of(address(col, h, first[col], core, second[col], 0), block_rows[col])
        wait_bytes(total.at[pl.ds(0, (nz - 1) * unit)], az_recv.at[col, h])
        for t in range(n - 1):
            s = lax.rem(second[col] + far(n, t), n)
            remote(total.at[block], total.at[block], ay_send.at[col, h], ay_recv.at[col, h], dev_second(col, s)).start()

    def pair_send_block(h, col, k, rows):
        remote(total.at[rows], total.at[rows], pair_send.at[col, h, k], pair_recv.at[col, h, k],
               dev(x, y, z, 1 - core)).start()

    def stage_ay(h, col):
        n, n1 = n_second[col], n_first[col]
        wait_bytes(total.at[pl.ds(0, (n - 1) * block_rows[col])], ay_recv.at[col, h])
        whole = rows_of(address(col, h, first[col], core, 0, 0), width)
        for d, step in enumerate((1, n1 - 1)):
            f = lax.rem(first[col] + step, n1)
            remote(total.at[whole], total.at[whole], ax_send.at[col, h, d], ax_recv.at[col, h, d],
                   dev_first(col, f, core)).start()
        pair_send_block(h, col, 0, whole)

    def stage_ax(h, col):
        n1 = n_first[col]
        for d, step in enumerate((1, n1 - 1)):
            src = lax.rem(first[col] + n1 - step, n1)
            nxt = lax.rem(first[col] + step, n1)
            whole = rows_of(address(col, h, src, core, 0, 0), width)
            wait_bytes(total.at[whole], ax_recv.at[col, h, d])
            part = rows_of(address(col, h, src, core, 0, 0) + d * (width // 2), width // 2)
            remote(total.at[part], total.at[part], af_send.at[col, h, d], af_recv.at[col, h, d],
                   dev_first(col, nxt, core)).start()
            pair_send_block(h, col, 1 + d, whole)

    def stage_af(h, col):
        n1 = n_first[col]
        src = lax.rem(first[col] + n1 // 2, n1)
        for d in range(2):
            part = rows_of(address(col, h, src, core, 0, 0) + d * (width // 2), width // 2)
            wait_bytes(total.at[part], af_recv.at[col, h, d])
            pair_send_block(h, col, 3 + d, part)

    def loss_stage(k):
        if k == 0:
            wait_bytes(loss_buf.at[0, pl.ds(0, members[0] - 1)], l_recv.at[0])
            loss_buf[1, y] = jnp.sum(loss_buf[0, pl.ds(0, members[0])], axis=0)
            for t in range(1, ny):
                remote(loss_buf.at[1, y], loss_buf.at[1, y], l_send.at[1], l_recv.at[1],
                       dev(x, lax.rem(y + t, ny), z, core)).start()
        elif k == 1:
            wait_bytes(loss_buf.at[1, pl.ds(0, ny - 1)], l_recv.at[1])
            loss_buf[2, z] = jnp.sum(loss_buf[1, pl.ds(0, ny)], axis=0)
            for t in range(1, nz):
                remote(loss_buf.at[2, z], loss_buf.at[2, z], l_send.at[2], l_recv.at[2],
                       dev(x, y, lax.rem(z + t, nz), core)).start()
        else:
            wait_bytes(loss_buf.at[2, pl.ds(0, nz - 1)], l_recv.at[2])
            loss_out[...] = jnp.sum(loss_buf[2, pl.ds(0, nz)], axis=0)

    stages = [(stage_g, 0), (stage_y, 5), (stage_z, 10), (stage_az, 15), (stage_ay, 20), (stage_ax, 26), (stage_af, 30)]
    plan = sorted(((at + 6 * h, k, h, col) for k, (_, at) in enumerate(stages) for h, col in order))
    for _, k, h, col in plan:
        stages[k][0](h, col)
        if (h, col) == (1, 1) and k < 3:
            loss_stage(k)

    for h, col in order:
        n1 = n_first[col]
        for k, src, off, n in (
            (0, first[col], 0, width),
            (1, lax.rem(first[col] + n1 - 1, n1), 0, width),
            (2, lax.rem(first[col] + 1, n1), 0, width),
            (3, lax.rem(first[col] + n1 // 2, n1), 0, width // 2),
            (4, lax.rem(first[col] + n1 // 2, n1), width // 2, width // 2),
        ):
            rows = rows_of(address(col, h, src, 1 - core, 0, 0) + off, n)
            wait_bytes(total.at[rows], pair_recv.at[col, h, k])
            wait_bytes(total.at[rows], pair_send.at[col, h, k])

    for col in range(2):
        wait_bytes(z_buf.at[col, pl.ds(0, members[col] - 1)], z_send.at[col])
        for h in range(halves):
            wait_bytes(g_buf.at[col, h, pl.ds(0, members[col] - 1)], g_send.at[col, h])
            wait_bytes(y_buf.at[col, h, pl.ds(0, n_second[col] - 1)], p_send.at[col, h])
            wait_bytes(sums.at[col, h, pl.ds(0, nz - 1)], s_send.at[col, h])
            wait_bytes(total.at[pl.ds(0, (nz - 1) * unit)], az_send.at[col, h])
            wait_bytes(total.at[pl.ds(0, (n_second[col] - 1) * block_rows[col])], ay_send.at[col, h])
            for d in range(2):
                wait_bytes(total.at[pl.ds(0, width)], ax_send.at[col, h, d])
                wait_bytes(total.at[pl.ds(0, width // 2)], af_send.at[col, h, d])
    wait_bytes(loss_buf.at[0, pl.ds(0, members[0] - 1)], l_send.at[0])
    wait_bytes(loss_buf.at[1, pl.ds(0, ny - 1)], l_send.at[1])
    wait_bytes(loss_buf.at[2, pl.ds(0, nz - 1)], l_send.at[2])


def sum_protos(nz, ny, nx, grads, z_rows, loss):
    blocks, rows, width = grads.shape
    dim = z_rows.shape[1]
    count = blocks * width
    members = nx * CORES
    any_spec = pl.BlockSpec(memory_space=pl.ANY)
    vmem = pl.BlockSpec(memory_space=pltpu.VMEM)
    dma = pltpu.SemaphoreType.DMA
    two = dma((2, 2))
    return pl.pallas_call(
        functools.partial(protos_kernel, nz, ny, nx),
        out_shape=(jax.ShapeDtypeStruct((count, dim), F32), jax.ShapeDtypeStruct((1, LANES), F32)),
        in_specs=[any_spec, any_spec, any_spec],
        out_specs=(vmem, vmem),
        scratch_shapes=[
            pltpu.VMEM((2, 2, members, rows, width), jnp.bfloat16),
            pltpu.VMEM((2, members, rows, dim), jnp.bfloat16),
            pltpu.VMEM((2, 2, width, dim), F32),
            pltpu.VMEM((2, 2, ny, width // ny, dim), F32),
            pltpu.VMEM((2, 2, 1, width // ny, dim), F32),
            pltpu.VMEM((2, 2, nz, width // ny // nz, dim), F32),
            pltpu.VMEM((3, max(members, nz), 1, LANES), F32),
            dma((7,)),
            dma((2,)), dma((2,)),
            two, two, two, two, two, two, two, two, two, two,
            dma((2, 2, 2)), dma((2, 2, 2)), dma((2, 2, 2)), dma((2, 2, 2)),
            dma((2, 2, 5)), dma((2, 2, 5)),
            dma((2,)),
            dma((3,)), dma((3,)),
        ],
        compiler_params=pltpu.CompilerParams(
            collective_id=1, has_side_effects=True, vmem_limit_bytes=48 * 2 ** 20),
        name="protos",
    )(grads, z_rows, loss)


def solution(mesh, nz=CHIPS_Z, nx=CHIPS_X):
    group_size = mesh.shape["data"]
    plane = group_size // (nz * CORES)
    ny = plane // nx

    def local_step(z_one, z_two, protos, queue_one, queue_two):
        batch_total = group_size * z_one.shape[0]
        scales = column_scales(nz, plane, z_one, z_two, queue_one, queue_two, protos)
        grad_coef = 1.0 / (2 * batch_total * TEMPERATURE)
        codes_one, codes_two, grads, dz_one, dz_two, loss = batch_codes(
            4 * nx * CORES, grad_coef, z_one, z_two, protos, scales)
        z_rows = jnp.concatenate([z_one, z_two], axis=0)
        grad_protos, loss = sum_protos(nz, ny, nx, grads, z_rows, loss)
        swap_loss = -jnp.sum(loss) / (2 * batch_total)
        return codes_one, codes_two, swap_loss, dz_one, dz_two, grad_protos

    row_spec = P("data", None)
    full_spec = P(None, None)
    return jax.shard_map(
        local_step,
        mesh=mesh,
        in_specs=(row_spec, row_spec, full_spec, row_spec, row_spec),
        out_specs=(row_spec, row_spec, P(), row_spec, row_spec, full_spec),
        check_vma=False,
    )
```

```python
import functools

import jax
import jax.numpy as jnp
from jax import lax
from jax.experimental import pallas as pl
from jax.experimental.pallas import tpu as pltpu
from jax.sharding import PartitionSpec as P

EPSILON = 0.05
TEMPERATURE = 0.1
ITERS = 3
CORES = 2
CHIPS_Z = 8
CHIPS_X = 4
VMEM_TOTAL = 67043328
LANES = 128
HALVES = 2
LOG2E = 1.4426950408889634
F32 = jnp.float32
BF16 = jnp.bfloat16
MESH = pl.DeviceIdType.MESH


def dot_nt(a, b):
    return lax.dot_general(a, b, (((1,), (1,)), ((), ())), preferred_element_type=F32)


def near_offset(k):
    return lax.div(k + 1, 2) * (2 * lax.rem(k, 2) - 1)


def far_first(n):
    return sorted(range(1, n), key=lambda d: (-min(d, n - d), d))


def remote(src, dst, send, recv, device):
    return pltpu.make_async_remote_copy(
        src_ref=src, dst_ref=dst, send_sem=send, recv_sem=recv, device_id=(device,), device_id_type=MESH)


def wait_bytes(ref, sem):
    pltpu.make_async_copy(ref, ref, sem).wait()


def step_kernel(
    nz, ny, nx, total_rows, protos_count, grad_coef, loss_coef,
    z_one, z_two, q_one, q_two, protos,
    codes_one, codes_two, loss_out, dz_one, dz_two, total,
    rows, cols, mat, wacc, rscale, csum, rs_buf, ex_buf, ag_buf,
    grads, g_buf, z_buf, part_buf, y_buf, yz_buf, sums, loss_buf,
    row_sem, col_sem, rs_send, rs_recv, ex_send, ex_recv, ag_send, ag_recv,
    z_send, z_recv, g_send, g_recv, p_send, p_recv, s_send, s_recv,
    az_send, az_recv, ay_send, ay_recv, ax_send, ax_recv, af_send, af_recv, pair_send, pair_recv,
    l_send, l_recv,
):
    me = lax.axis_index("data")
    core = lax.rem(me, CORES)
    chip = lax.div(me, CORES)
    plane = nx * ny
    yx = lax.rem(chip, plane)
    z = lax.div(chip, plane)
    x = lax.rem(yx, nx)
    y = lax.div(yx, nx)

    def dev(xx, yy, z2, cc):
        return ((z2 * ny + yy) * nx + xx) * CORES + cc

    members = nz * CORES
    mine = z * CORES + core
    tiles = mat.shape[1]
    per = tiles // members
    n_rows = mat.shape[2]
    batch = z_one.shape[0]
    wide = per * LANES
    blocks = 3 if n_rows % 24 == 0 else 1
    rb = n_rows // blocks
    unroll = 2

    def near(t):
        zz = lax.rem(z + near_offset(lax.div(t, 2)) + nz, nz)
        return zz * CORES + lax.rem(core + lax.rem(t, 2), CORES)

    member_offsets = [(dz, e) for dz in far_first(nz) for e in range(CORES)] + [(0, 1)]

    def member_at(dz, e):
        zz, cc = lax.rem(z + dz, nz), lax.rem(core + e, CORES)
        return zz * CORES + cc, dev(x, y, zz, cc)

    plane_offsets = [(dy, dx) for dy in range(ny) for dx in range(nx)][1:]
    plane_offsets.sort(key=lambda o: -(min(o[0], ny - o[0]) + min(o[1], nx - o[1])))

    def plane_at(dy, dx):
        yy, xx = lax.rem(y + dy, ny), lax.rem(x + dx, nx)
        return dev(xx, yy, z, core)

    views = ((z_one, q_one), (z_two, q_two))
    row_copies = [
        [pltpu.make_async_copy(zr, rows.at[v, pl.ds(0, batch)], row_sem.at[v, 0]),
         pltpu.make_async_copy(qr, rows.at[v, pl.ds(batch, n_rows - batch)], row_sem.at[v, 1])]
        for v, (zr, qr) in enumerate(views)]

    def slice_cols(m):
        return pl.ds(pl.multiple_of(m * wide, wide), wide)

    def col_copy(m):
        return pltpu.make_async_copy(protos.at[slice_cols(m)], cols.at[slice_cols(m)], col_sem.at[m])

    for c in row_copies[0]:
        c.start()
    for dz, e in member_offsets:
        col_copy(member_at(dz, e)[0]).start()
    col_copy(mine).start()
    for c in row_copies[1]:
        c.start()

    barrier = pltpu.get_barrier_semaphore()
    reached = [member_at(dz, e)[1] for dz, e in member_offsets] + [plane_at(*o) for o in plane_offsets]
    reached += [dev(lax.rem(x + d, nx), y, z, 1 - core) for d in range(1, nx)]
    reached += [dev(x, lax.rem(y + d, ny), z, 1 - core) for d in range(1, ny)]
    for device in reached:
        pl.semaphore_signal(barrier, inc=1, device_id=(device,), device_id_type=MESH)

    def rs_start(it, v, m, device):
        remote(csum.at[it, v, m], rs_buf.at[it, v, mine], rs_send.at[it, v], rs_recv.at[it, v], device).start()

    def rs_start_all(it, v):
        for dz, e in member_offsets:
            rs_start(it, v, *member_at(dz, e))

    def first_pass(v):
        for c in row_copies[v]:
            c.wait()

        def step(t, carry):
            ms = [near(members - 1 - (t * unroll + u)) for u in range(unroll)]
            if v == 0:
                for m in ms:
                    col_copy(m).wait()
            for m in ms:
                scores = dot_nt(rows[v], cols[slice_cols(m), :])
                for j in range(per):
                    e = jnp.exp2(scores[:, j * LANES:(j + 1) * LANES] * (LOG2E / EPSILON))
                    mat[v, m * per + j] = e
                    csum[0, v, m, pl.ds(j, 1), :] = jnp.sum(e, axis=0, keepdims=True)
            return carry

        lax.fori_loop(0, members // unroll, step, 0)

    first_pass(0)
    pl.semaphore_wait(barrier, len(reached))
    rs_start_all(0, 0)
    first_pass(1)
    rs_start_all(0, 1)

    def reduce_slice(it, v):
        wait_bytes(rs_buf.at[it, v, pl.ds(0, members - 1)], rs_recv.at[it, v])
        rs_buf[it, v, mine] = csum[it, v, mine]
        ex_buf[it, v, yx] = jnp.sum(rs_buf[it, v], axis=0)
        for o in plane_offsets:
            remote(ex_buf.at[it, v, yx], ex_buf.at[it, v, yx], ex_send.at[it, v], ex_recv.at[it, v], plane_at(*o)).start()

    def share_scale(it, v):
        wait_bytes(ex_buf.at[it, v, pl.ds(0, plane - 1)], ex_recv.at[it, v])
        ag_buf[it, v, mine] = 1.0 / (protos_count * jnp.sum(ex_buf[it, v], axis=0))
        for dz, e in member_offsets:
            remote(ag_buf.at[it, v, mine], ag_buf.at[it, v, mine], ag_send.at[it, v], ag_recv.at[it, v, mine],
                   member_at(dz, e)[1]).start()

    def wait_scale(it, v, m):
        wait_bytes(ag_buf.at[it, v, m], ag_recv.at[it, v, m])

    def next_pass(it, v):
        wacc[...] = jnp.zeros_like(wacc)

        def add_slice(t, carry):
            m = near(t)

            @pl.when(t > 0)
            def _():
                wait_scale(it, v, m)

            for b in range(blocks):
                part = pl.ds(b * rb, rb)
                acc = wacc[part, :]
                for j in range(per):
                    acc += mat[v, m * per + j, part, :] * ag_buf[it, v, m, pl.ds(j, 1), :]
                wacc[part, :] = acc
            return carry

        lax.fori_loop(0, members, add_slice, 0)
        row_sum = jnp.sum(wacc[...], axis=1, keepdims=True)
        rscale[...] = jnp.broadcast_to(1.0 / (total_rows * row_sum), rscale.shape)

        def col_slice(t, carry):
            m = near(members - 1 - t)
            acc = [None] * per
            for b in range(blocks):
                part = pl.ds(b * rb, rb)
                r = rscale[part, :]
                for j in range(per):
                    p = (mat[v, m * per + j, part, :] * r).reshape(rb // 8, 8, LANES).sum(axis=0)
                    acc[j] = p if acc[j] is None else acc[j] + p
            for j in range(per):
                csum[it + 1, v, m, pl.ds(j, 1), :] = jnp.sum(acc[j], axis=0, keepdims=True)

            @pl.when(t > 0)
            def _():
                before = near(members - t)
                rs_start(it + 1, v, before, dev(x, y, lax.div(before, CORES), lax.rem(before, CORES)))
            return carry

        lax.fori_loop(0, members, col_slice, 0)

    codes_refs = (codes_one, codes_two)
    width = g_buf.shape[4]
    chunks = grads.shape[0]

    def chunk_cols(t):
        return pl.ds(pl.multiple_of(t * width, width), width)

    def lane_fold(a):
        return sum(a[:, j:j + LANES] for j in range(0, a.shape[1], LANES))

    def softmax_terms(v):
        def step(t, acc):
            terms = jnp.exp2(dot_nt(rows[v, pl.ds(0, batch), :], cols[slice_cols(t), :]) * (LOG2E / TEMPERATURE))
            codes_refs[v][:, slice_cols(t)] = terms
            return acc + lane_fold(terms)
        acc = lax.fori_loop(0, members, step, jnp.zeros((batch, LANES), F32))
        return jnp.sum(acc, axis=1, keepdims=True)

    n_first, n_second = (nx, ny), (ny, nx)
    first, second = (x, y), (y, x)
    slot = [first[col] * CORES + core for col in range(2)]
    group = [n_first[col] * CORES for col in range(2)]

    def dev_first(col, f, cc):
        return dev(f, y, z, cc) if col == 0 else dev(x, f, z, cc)

    def dev_second(col, s):
        return dev(x, s, z, core) if col == 0 else dev(s, y, z, core)

    def first_offsets(col):
        return [(d, c) for d in far_first(n_first[col]) for c in range(CORES)] + [(0, 1)]

    def first_at(col, d, c):
        f, cc = lax.rem(first[col] + d, n_first[col]), lax.rem(core + c, CORES)
        return f * CORES + cc, dev_first(col, f, cc)

    def share_rows():
        for col in range(2):
            for v in range(2):
                z_buf[col, slot[col], pl.ds(v * batch, batch), :] = rows[v, pl.ds(0, batch), :]
            for o in first_offsets(col):
                for v in range(2):
                    remote(rows.at[v, pl.ds(0, batch)], z_buf.at[col, slot[col], pl.ds(v * batch, batch)],
                           z_send.at[col], z_recv.at[col], first_at(col, *o)[1]).start()

    share_rows()
    reduce_slice(0, 0)
    prob_sum = [softmax_terms(0)]
    reduce_slice(0, 1)
    share_scale(0, 0)
    prob_sum.append(softmax_terms(1))
    share_scale(0, 1)

    def iteration(it, carry):
        for v in range(2):
            next_pass(it, v)
        for v in range(2):
            reduce_slice(it + 1, v)
        for v in range(2):
            share_scale(it + 1, v)
        return carry

    lax.fori_loop(0, ITERS - 1, iteration, 0)
    last = ITERS - 1

    top = pl.ds(0, batch)

    def scaled(v, j):
        return mat[v, j, top, :] * ag_buf[last, v, lax.div(j, per), pl.ds(lax.rem(j, per), 1), :]

    def plan_sum(v):
        def step(t, acc):
            m = near(t)

            @pl.when(t > 0)
            def _():
                wait_scale(last, v, m)
            return acc + sum(mat[v, m * per + j, top, :] * ag_buf[last, v, m, pl.ds(j, 1), :] for j in range(per))
        acc = lax.fori_loop(0, members, step, jnp.zeros((batch, LANES), F32))
        return jnp.sum(acc, axis=1, keepdims=True)

    plan_inv = [1.0 / plan_sum(v) for v in range(2)]
    code_coef = [jnp.broadcast_to(plan_inv[v] * grad_coef, (batch, LANES)) for v in range(2)]
    prob_coef = [jnp.broadcast_to(grad_coef / prob_sum[v], (batch, LANES)) for v in range(2)]
    spread = width // LANES

    def g_start(col, h, m, device):
        block = (col * group[col] + m) * HALVES + h
        remote(grads.at[block], g_buf.at[col, h, slot[col]], g_send.at[col, h], g_recv.at[col, h], device).start()

    order = [(h, col) for h in range(HALVES) for col in range(2)]
    for h, col in order:
        def exchange_member(k):
            f = lax.rem(first[col] + near_offset(lax.div(k, 2)) + n_first[col], n_first[col])
            return f, lax.rem(core + lax.rem(k, 2), CORES)

        def make_block(t, carry, h=h, col=col, exchange_member=exchange_member):
            f, cc = exchange_member(group[col] - 1 - t)
            m = f * CORES + cc
            block = (col * group[col] + m) * HALVES + h
            for i in range(spread):
                j = block * spread + i
                lanes = pl.ds(pl.multiple_of(j * LANES, LANES), LANES)
                plans = [scaled(v, j) * code_coef[v] for v in range(2)]
                for v in range(2):
                    g = codes_refs[v][:, lanes] * prob_coef[v] - plans[1 - v]
                    grads[block, pl.ds(v * batch, batch), pl.ds(i * LANES, LANES)] = g.astype(BF16)

            @pl.when(t > 0)
            def _():
                f, cc = exchange_member(group[col] - t)
                g_start(col, h, f * CORES + cc, dev_first(col, f, cc))
            return carry

        lax.fori_loop(0, group[col], make_block, 0)
        g_buf[col, h, slot[col]] = grads[(col * group[col] + slot[col]) * HALVES + h]

    lse = [jnp.log(prob_sum[v]) for v in range(2)]

    def finish(t, carry):
        loss, dz = carry
        scores = [dot_nt(rows[v, top, :], cols[chunk_cols(t), :]) for v in range(2)]
        for i in range(spread):
            j = t * spread + i
            lanes = pl.ds(pl.multiple_of(j * LANES, LANES), LANES)
            for v in range(2):
                codes = scaled(v, j) * plan_inv[v]
                codes_refs[v][:, lanes] = codes
                other = scores[1 - v][:, i * LANES:(i + 1) * LANES]
                loss = loss + codes * (other * (1.0 / TEMPERATURE) - lse[1 - v])
        dz = dz + jnp.dot(grads[t], cols[chunk_cols(t), :], preferred_element_type=F32)
        return loss, dz

    loss, dz = lax.fori_loop(0, chunks, finish, (jnp.zeros((batch, LANES), F32), jnp.zeros((2 * batch, cols.shape[1]), F32)))
    dz_one[...] = dz[:batch]
    dz_two[...] = dz[batch:]
    loss_buf[0, slot[0]] = jnp.sum(loss, axis=0, keepdims=True)
    for o in first_offsets(0):
        remote(loss_buf.at[0, slot[0]], loss_buf.at[0, slot[0]], l_send.at[0], l_recv.at[0], first_at(0, *o)[1]).start()

    block_rows = [width // n_second[col] for col in range(2)]
    unit = block_rows[0] // nz

    def address(col, h, f, cc, s, zi):
        half_count = total.shape[0] // 2
        return col * half_count + ((f * CORES + cc) * HALVES + h) * width + s * block_rows[col] + zi * unit

    def rows_of(addr, n):
        return pl.ds(pl.multiple_of(addr, 8), n)

    def stage_g(h, col):
        wait_bytes(g_buf.at[col, h, pl.ds(0, group[col] - 1)], g_recv.at[col, h])
        if h == 0:
            wait_bytes(z_buf.at[col, pl.ds(0, group[col] - 1)], z_recv.at[col])
        k = group[col] * z_buf.shape[2]
        g = g_buf[col, h].reshape(k, width)
        zs = z_buf[col].reshape(k, z_buf.shape[3])
        part_buf[col, h] = lax.dot_general(g, zs, (((0,), (0,)), ((), ())), preferred_element_type=F32)
        for d in far_first(n_second[col]):
            s = lax.rem(second[col] + d, n_second[col])
            remote(part_buf.at[col, h, rows_of(s * block_rows[col], block_rows[col])], y_buf.at[col, h, second[col]],
                   p_send.at[col, h], p_recv.at[col, h], dev_second(col, s)).start()

    def stage_y(h, col):
        wait_bytes(y_buf.at[col, h, pl.ds(0, n_second[col] - 1)], p_recv.at[col, h])
        y_buf[col, h, second[col]] = part_buf[col, h, rows_of(second[col] * block_rows[col], block_rows[col])]
        yz_buf[col, h, 0] = jnp.sum(y_buf[col, h], axis=0)
        for d in far_first(nz):
            z2 = lax.rem(z + d, nz)
            remote(yz_buf.at[col, h, 0, rows_of(z2 * unit, unit)], sums.at[col, h, z],
                   s_send.at[col, h], s_recv.at[col, h], dev(x, y, z2, core)).start()

    def stage_z(h, col):
        wait_bytes(sums.at[col, h, pl.ds(0, nz - 1)], s_recv.at[col, h])
        sums[col, h, z] = yz_buf[col, h, 0, rows_of(z * unit, unit)]
        own = rows_of(address(col, h, first[col], core, second[col], z), unit)
        total[own, :] = jnp.sum(sums[col, h], axis=0)
        for d in far_first(nz):
            z2 = lax.rem(z + d, nz)
            remote(total.at[own], total.at[own], az_send.at[col, h], az_recv.at[col, h], dev(x, y, z2, core)).start()

    def stage_az(h, col):
        block = rows_of(address(col, h, first[col], core, second[col], 0), block_rows[col])
        wait_bytes(total.at[pl.ds(0, (nz - 1) * unit)], az_recv.at[col, h])
        for d in far_first(n_second[col]):
            s = lax.rem(second[col] + d, n_second[col])
            remote(total.at[block], total.at[block], ay_send.at[col, h], ay_recv.at[col, h], dev_second(col, s)).start()

    def pair_start(h, col, k, part):
        remote(total.at[part], total.at[part], pair_send.at[col, h, k], pair_recv.at[col, h, k],
               dev(x, y, z, 1 - core)).start()

    def stage_ay(h, col):
        n1 = n_first[col]
        wait_bytes(total.at[pl.ds(0, (n_second[col] - 1) * block_rows[col])], ay_recv.at[col, h])
        whole = rows_of(address(col, h, first[col], core, 0, 0), width)
        for d, step in enumerate((1, n1 - 1)):
            f = lax.rem(first[col] + step, n1)
            remote(total.at[whole], total.at[whole], ax_send.at[col, h, d], ax_recv.at[col, h, d],
                   dev_first(col, f, core)).start()
        pair_start(h, col, 0, whole)

    def stage_ax(h, col):
        n1 = n_first[col]
        for d, step in enumerate((1, n1 - 1)):
            src = lax.rem(first[col] + n1 - step, n1)
            nxt = lax.rem(first[col] + step, n1)
            whole = rows_of(address(col, h, src, core, 0, 0), width)
            wait_bytes(total.at[whole], ax_recv.at[col, h, d])
            part = rows_of(address(col, h, src, core, 0, 0) + d * (width // 2), width // 2)
            remote(total.at[part], total.at[part], af_send.at[col, h, d], af_recv.at[col, h, d],
                   dev_first(col, nxt, core)).start()
            pair_start(h, col, 1 + d, whole)

    def stage_af(h, col):
        n1 = n_first[col]
        src = lax.rem(first[col] + n1 // 2, n1)
        for d in range(2):
            part = rows_of(address(col, h, src, core, 0, 0) + d * (width // 2), width // 2)
            wait_bytes(total.at[part], af_recv.at[col, h, d])
            pair_start(h, col, 3 + d, part)

    def loss_stage(k):
        if k == 0:
            wait_bytes(loss_buf.at[0, pl.ds(0, group[0] - 1)], l_recv.at[0])
            loss_buf[1, y] = jnp.sum(loss_buf[0, pl.ds(0, group[0])], axis=0)
            for d in range(1, ny):
                remote(loss_buf.at[1, y], loss_buf.at[1, y], l_send.at[1], l_recv.at[1],
                       dev(x, lax.rem(y + d, ny), z, core)).start()
        elif k == 1:
            wait_bytes(loss_buf.at[1, pl.ds(0, ny - 1)], l_recv.at[1])
            loss_buf[2, z] = jnp.sum(loss_buf[1, pl.ds(0, ny)], axis=0)
            for d in range(1, nz):
                remote(loss_buf.at[2, z], loss_buf.at[2, z], l_send.at[2], l_recv.at[2],
                       dev(x, y, lax.rem(z + d, nz), core)).start()
        else:
            wait_bytes(loss_buf.at[2, pl.ds(0, nz - 1)], l_recv.at[2])
            terms = jnp.sum(loss_buf[2, pl.ds(0, nz)], axis=0)
            loss_out[...] = jnp.sum(terms, axis=1, keepdims=True) * loss_coef

    stages = [(stage_g, 0), (stage_y, 5), (stage_z, 10), (stage_az, 15), (stage_ay, 20), (stage_ax, 26), (stage_af, 30)]
    steps = sorted((at + 6 * h, k, h, col) for k, (_, at) in enumerate(stages) for h, col in order)
    for _, k, h, col in steps:
        stages[k][0](h, col)
        if (h, col) == (1, 1) and k < 3:
            loss_stage(k)

    for h, col in order:
        n1 = n_first[col]
        for k, src, off, n in (
            (0, first[col], 0, width),
            (1, lax.rem(first[col] + n1 - 1, n1), 0, width),
            (2, lax.rem(first[col] + 1, n1), 0, width),
            (3, lax.rem(first[col] + n1 // 2, n1), 0, width // 2),
            (4, lax.rem(first[col] + n1 // 2, n1), width // 2, width // 2),
        ):
            part = rows_of(address(col, h, src, 1 - core, 0, 0) + off, n)
            wait_bytes(total.at[part], pair_recv.at[col, h, k])
            wait_bytes(total.at[part], pair_send.at[col, h, k])

    def drain(it, carry):
        for v in range(2):
            wait_bytes(rs_buf.at[it, v, pl.ds(0, members - 1)], rs_send.at[it, v])
            wait_bytes(ex_buf.at[it, v, pl.ds(0, plane - 1)], ex_send.at[it, v])
            wait_bytes(rs_buf.at[it, v, pl.ds(0, members - 1)], ag_send.at[it, v])
        return carry

    lax.fori_loop(0, ITERS, drain, 0)
    for col in range(2):
        wait_bytes(z_buf.at[col, pl.ds(0, group[col] - 1)], z_send.at[col])
        for h in range(HALVES):
            wait_bytes(g_buf.at[col, h, pl.ds(0, group[col] - 1)], g_send.at[col, h])
            wait_bytes(y_buf.at[col, h, pl.ds(0, n_second[col] - 1)], p_send.at[col, h])
            wait_bytes(sums.at[col, h, pl.ds(0, nz - 1)], s_send.at[col, h])
            wait_bytes(total.at[pl.ds(0, (nz - 1) * unit)], az_send.at[col, h])
            wait_bytes(total.at[pl.ds(0, (n_second[col] - 1) * block_rows[col])], ay_send.at[col, h])
            for d in range(2):
                wait_bytes(total.at[pl.ds(0, width)], ax_send.at[col, h, d])
                wait_bytes(total.at[pl.ds(0, width // 2)], af_send.at[col, h, d])
    wait_bytes(loss_buf.at[0, pl.ds(0, group[0] - 1)], l_send.at[0])
    wait_bytes(loss_buf.at[1, pl.ds(0, ny - 1)], l_send.at[1])
    wait_bytes(loss_buf.at[2, pl.ds(0, nz - 1)], l_send.at[2])


def fused_step(nz, ny, nx, z_one, z_two, q_one, q_two, protos):
    batch, dim = z_one.shape
    n_rows = batch + q_one.shape[0]
    count = protos.shape[0]
    tiles = count // LANES
    members = nz * CORES
    plane = nx * ny
    devices = plane * members
    small = (tiles // members, LANES)
    group = nx * CORES
    chunks = 2 * HALVES * group
    width = count // chunks
    any_spec = pl.BlockSpec(memory_space=pl.ANY)
    vmem = pl.BlockSpec(memory_space=pltpu.VMEM)
    dma = pltpu.SemaphoreType.DMA
    two = dma((2, HALVES))
    out_bytes = 4 * (2 * batch * count + 2 * batch * dim + count * dim)
    return pl.pallas_call(
        functools.partial(
            step_kernel, nz, ny, nx, float(devices * n_rows), float(count),
            1.0 / (2 * devices * batch * TEMPERATURE), -1.0 / (2 * devices * batch)),
        out_shape=(
            pltpu.VMEM((batch, count), F32),
            pltpu.VMEM((batch, count), F32),
            pltpu.VMEM((1, 1), F32),
            pltpu.VMEM((batch, dim), F32),
            pltpu.VMEM((batch, dim), F32),
            pltpu.VMEM((count, dim), F32),
        ),
        in_specs=[any_spec] * 5,
        out_specs=(vmem,) * 6,
        scratch_shapes=[
            pltpu.VMEM((2, n_rows, dim), BF16),
            pltpu.VMEM((count, dim), BF16),
            pltpu.VMEM((2, tiles, n_rows, LANES), F32),
            pltpu.VMEM((n_rows, LANES), F32),
            pltpu.VMEM((n_rows, LANES), F32),
            pltpu.VMEM((ITERS, 2, members) + small, F32),
            pltpu.VMEM((ITERS, 2, members) + small, F32),
            pltpu.VMEM((ITERS, 2, plane) + small, F32),
            pltpu.VMEM((ITERS, 2, members) + small, F32),
            pltpu.VMEM((chunks, 2 * batch, width), BF16),
            pltpu.VMEM((2, HALVES, group, 2 * batch, width), BF16),
            pltpu.VMEM((2, group, 2 * batch, dim), BF16),
            pltpu.VMEM((2, HALVES, width, dim), F32),
            pltpu.VMEM((2, HALVES, ny, width // ny, dim), F32),
            pltpu.VMEM((2, HALVES, 1, width // ny, dim), F32),
            pltpu.VMEM((2, HALVES, nz, width // ny // nz, dim), F32),
            pltpu.VMEM((3, max(group, nz), 1, LANES), F32),
            dma((2, 2)),
            dma((members,)),
            dma((ITERS, 2)), dma((ITERS, 2)), dma((ITERS, 2)), dma((ITERS, 2)), dma((ITERS, 2)),
            dma((ITERS, 2, members)),
            dma((2,)), dma((2,)),
            two, two, two, two, two, two, two, two, two, two,
            dma((2, HALVES, 2)), dma((2, HALVES, 2)), dma((2, HALVES, 2)), dma((2, HALVES, 2)),
            dma((2, HALVES, 5)), dma((2, HALVES, 5)),
            dma((3,)), dma((3,)),
        ],
        compiler_params=pltpu.CompilerParams(
            collective_id=0, has_side_effects=True, vmem_limit_bytes=VMEM_TOTAL - out_bytes - 2 ** 16),
        name="step",
    )(z_one, z_two, q_one, q_two, protos)


def flush(arrays):
    n = len(arrays)

    def kernel(*refs):
        sem = refs[-1]
        copies = [pltpu.make_async_copy(refs[i], refs[n + i], sem.at[i]) for i in range(n)]
        for c in copies:
            c.start()
        for c in copies:
            c.wait()

    return pl.pallas_call(
        kernel,
        out_shape=tuple(jax.ShapeDtypeStruct(a.shape, a.dtype) for a in arrays),
        in_specs=[pl.BlockSpec(memory_space=pltpu.VMEM)] * n,
        out_specs=(pl.BlockSpec(memory_space=pltpu.HBM),) * n,
        scratch_shapes=[pltpu.SemaphoreType.DMA((n,))],
        compiler_params=pltpu.CompilerParams(vmem_limit_bytes=2 ** 20),
        name="flush",
    )(*(pltpu.with_memory_space_constraint(a, pltpu.VMEM) for a in arrays))


def solution(mesh, nz=CHIPS_Z, nx=CHIPS_X):
    ny = mesh.shape["data"] // (nz * nx * CORES)

    def local_step(z_one, z_two, protos, queue_one, queue_two):
        outs = fused_step(nz, ny, nx, z_one, z_two, queue_one, queue_two, protos)
        codes_one, codes_two, loss, dz_one, dz_two, grad_protos = flush(outs)
        return codes_one, codes_two, loss.reshape(()), dz_one, dz_two, grad_protos

    row_spec = P("data", None)
    full_spec = P(None, None)
    return jax.shard_map(
        local_step,
        mesh=mesh,
        in_specs=(row_spec, row_spec, full_spec, row_spec, row_spec),
        out_specs=(row_spec, row_spec, P(), row_spec, row_spec, full_spec),
        check_vma=False,
    )
```

```python
import functools

import jax
import jax.numpy as jnp
from jax import lax
from jax.experimental import pallas as pl
from jax.experimental.pallas import tpu as pltpu
from jax.sharding import PartitionSpec as P

EPSILON = 0.05
TEMPERATURE = 0.1
ITERS = 3
CORES = 2
CHIPS_Z = 8
CHIPS_X = 4
VMEM_TOTAL = 67043328
LANES = 128
HALVES = 2
LOG2E = 1.4426950408889634
F32 = jnp.float32
BF16 = jnp.bfloat16
MESH = pl.DeviceIdType.MESH


def dot_nt(a, b):
    return lax.dot_general(a, b, (((1,), (1,)), ((), ())), preferred_element_type=F32)


def near_offset(k):
    return lax.div(k + 1, 2) * (2 * lax.rem(k, 2) - 1)


def far_first(n):
    return sorted(range(1, n), key=lambda d: (-min(d, n - d), d))


def remote(src, dst, send, recv, device):
    return pltpu.make_async_remote_copy(
        src_ref=src, dst_ref=dst, send_sem=send, recv_sem=recv, device_id=(device,), device_id_type=MESH)


def wait_bytes(ref, sem):
    pltpu.make_async_copy(ref, ref, sem).wait()


def step_kernel(
    nz, ny, nx, total_rows, protos_count, grad_coef, loss_coef,
    z_one, z_two, q_one, q_two, protos,
    codes_one, codes_two, loss_out, dz_one, dz_two, total,
    rows, cols, mat, wacc, rscale, csum, rs_buf, ex_buf, ag_buf,
    grads, g_buf, z_buf, part_buf, y_buf, yz_buf, sums, loss_buf,
    row_sem, col_sem, rs_send, rs_recv, ex_send, ex_recv, ag_send, ag_recv,
    z_send, z_recv, g_send, g_recv, p_send, p_recv, s_send, s_recv,
    az_send, az_recv, ay_send, ay_recv, ax_send, ax_recv, af_send, af_recv, pair_send, pair_recv,
    l_send, l_recv,
):
    me = lax.axis_index("data")
    core = lax.rem(me, CORES)
    chip = lax.div(me, CORES)
    plane = nx * ny
    yx = lax.rem(chip, plane)
    z = lax.div(chip, plane)
    x = lax.rem(yx, nx)
    y = lax.div(yx, nx)

    def dev(xx, yy, z2, cc):
        return ((z2 * ny + yy) * nx + xx) * CORES + cc

    members = nz * CORES
    mine = z * CORES + core
    tiles = mat.shape[1]
    per = tiles // members
    n_rows = mat.shape[2]
    batch = z_one.shape[0]
    wide = per * LANES
    blocks = 3 if n_rows % 24 == 0 else 1
    rb = n_rows // blocks
    unroll = 4 if members % 4 == 0 else 1

    def near(t):
        zz = lax.rem(z + near_offset(lax.div(t, 2)) + nz, nz)
        return zz * CORES + lax.rem(core + lax.rem(t, 2), CORES)

    member_offsets = [(dz, e) for dz in far_first(nz) for e in range(CORES)] + [(0, 1)]

    def member_at(dz, e):
        zz, cc = lax.rem(z + dz, nz), lax.rem(core + e, CORES)
        return zz * CORES + cc, dev(x, y, zz, cc)

    plane_offsets = [(dy, dx) for dy in range(ny) for dx in range(nx)][1:]
    plane_offsets.sort(key=lambda o: -(min(o[0], ny - o[0]) + min(o[1], nx - o[1])))

    def plane_at(dy, dx):
        yy, xx = lax.rem(y + dy, ny), lax.rem(x + dx, nx)
        return dev(xx, yy, z, core)

    views = ((z_one, q_one), (z_two, q_two))
    row_copies = [
        [pltpu.make_async_copy(zr, rows.at[v, pl.ds(0, batch)], row_sem.at[v, 0]),
         pltpu.make_async_copy(qr, rows.at[v, pl.ds(batch, n_rows - batch)], row_sem.at[v, 1])]
        for v, (zr, qr) in enumerate(views)]

    def slice_cols(m):
        return pl.ds(pl.multiple_of(m * wide, wide), wide)

    def col_copy(m):
        return pltpu.make_async_copy(protos.at[slice_cols(m)], cols.at[slice_cols(m)], col_sem.at[m])

    for c in row_copies[0]:
        c.start()
    for dz, e in member_offsets:
        col_copy(member_at(dz, e)[0]).start()
    col_copy(mine).start()
    for c in row_copies[1]:
        c.start()

    barrier = pltpu.get_barrier_semaphore()
    reached = [member_at(dz, e)[1] for dz, e in member_offsets] + [plane_at(*o) for o in plane_offsets]
    reached += [dev(lax.rem(x + d, nx), y, z, 1 - core) for d in range(1, nx)]
    reached += [dev(x, lax.rem(y + d, ny), z, 1 - core) for d in range(1, ny)]
    for device in reached:
        pl.semaphore_signal(barrier, inc=1, device_id=(device,), device_id_type=MESH)

    def rs_start(it, v, m, device):
        remote(csum.at[it, v, m], rs_buf.at[it, v, mine], rs_send.at[it, v], rs_recv.at[it, v], device).start()

    def rs_start_all(it, v):
        for dz, e in member_offsets:
            rs_start(it, v, *member_at(dz, e))

    def first_pass(v):
        for c in row_copies[v]:
            c.wait()

        def step(t, carry):
            ms = [near(members - 1 - (t * unroll + u)) for u in range(unroll)]
            if v == 0:
                for m in ms:
                    col_copy(m).wait()
            for m in ms:
                scores = dot_nt(rows[v], cols[slice_cols(m), :])
                for j in range(per):
                    e = jnp.exp2(scores[:, j * LANES:(j + 1) * LANES] * (LOG2E / EPSILON))
                    mat[v, m * per + j] = e
                    csum[0, v, m, pl.ds(j, 1), :] = jnp.sum(e, axis=0, keepdims=True)
            return carry

        lax.fori_loop(0, members // unroll, step, 0)

    first_pass(0)
    pl.semaphore_wait(barrier, len(reached))
    rs_start_all(0, 0)
    first_pass(1)
    rs_start_all(0, 1)

    def reduce_slice(it, v):
        wait_bytes(rs_buf.at[it, v, pl.ds(0, members - 1)], rs_recv.at[it, v])
        rs_buf[it, v, mine] = csum[it, v, mine]
        ex_buf[it, v, yx] = jnp.sum(rs_buf[it, v], axis=0)
        for o in plane_offsets:
            remote(ex_buf.at[it, v, yx], ex_buf.at[it, v, yx], ex_send.at[it, v], ex_recv.at[it, v], plane_at(*o)).start()

    def share_scale(it, v):
        wait_bytes(ex_buf.at[it, v, pl.ds(0, plane - 1)], ex_recv.at[it, v])
        ag_buf[it, v, mine] = 1.0 / (protos_count * jnp.sum(ex_buf[it, v], axis=0))
        for dz, e in member_offsets:
            remote(ag_buf.at[it, v, mine], ag_buf.at[it, v, mine], ag_send.at[it, v], ag_recv.at[it, v, mine],
                   member_at(dz, e)[1]).start()

    def wait_scale(it, v, m):
        wait_bytes(ag_buf.at[it, v, m], ag_recv.at[it, v, m])

    def next_pass(it, v):
        def add_slice(m, fresh):
            for b in range(blocks):
                part = pl.ds(b * rb, rb)
                acc = None if fresh else wacc[part, :]
                for j in range(per):
                    term = mat[v, m * per + j, part, :] * ag_buf[it, v, m, pl.ds(j, 1), :]
                    acc = term if acc is None else acc + term
                wacc[part, :] = acc

        def add_next(t, m):
            wait_scale(it, v, m)
            add_slice(m, False)
            return near(t + 1)

        add_slice(mine, True)
        lax.fori_loop(1, members, add_next, near(1))
        row_sum = jnp.sum(wacc[...], axis=1, keepdims=True)
        rscale[...] = jnp.broadcast_to(1.0 / (total_rows * row_sum), rscale.shape)

        def col_slice(m):
            acc = [None] * per
            for b in range(blocks):
                part = pl.ds(b * rb, rb)
                r = rscale[part, :]
                for j in range(per):
                    p = (mat[v, m * per + j, part, :] * r).reshape(rb // 8, 8, LANES).sum(axis=0)
                    acc[j] = p if acc[j] is None else acc[j] + p
            for j in range(per):
                csum[it + 1, v, m, pl.ds(j, 1), :] = jnp.sum(acc[j], axis=0, keepdims=True)

        def col_next(t, carry):
            before, m = carry
            col_slice(m)
            rs_start(it + 1, v, before, dev(x, y, lax.div(before, CORES), lax.rem(before, CORES)))
            return m, near(members - 2 - t)

        col_slice(near(members - 1))
        lax.fori_loop(1, members, col_next, (near(members - 1), near(members - 2)))

    codes_refs = (codes_one, codes_two)
    width = g_buf.shape[4]
    chunks = grads.shape[0]

    def chunk_cols(t):
        return pl.ds(pl.multiple_of(t * width, width), width)

    def lane_fold(a):
        return sum(a[:, j:j + LANES] for j in range(0, a.shape[1], LANES))

    def softmax_terms(v):
        def step(t, acc):
            for u in range(2):
                part = slice_cols(t * 2 + u)
                terms = jnp.exp2(dot_nt(rows[v, pl.ds(0, batch), :], cols[part, :]) * (LOG2E / TEMPERATURE))
                codes_refs[v][:, part] = terms
                acc = acc + lane_fold(terms)
            return acc
        acc = lax.fori_loop(0, members // 2, step, jnp.zeros((batch, LANES), F32))
        return jnp.sum(acc, axis=1, keepdims=True)

    n_first, n_second = (nx, ny), (ny, nx)
    first, second = (x, y), (y, x)
    slot = [first[col] * CORES + core for col in range(2)]
    group = [n_first[col] * CORES for col in range(2)]

    def dev_first(col, f, cc):
        return dev(f, y, z, cc) if col == 0 else dev(x, f, z, cc)

    def dev_second(col, s):
        return dev(x, s, z, core) if col == 0 else dev(s, y, z, core)

    def first_offsets(col):
        return [(d, c) for d in far_first(n_first[col]) for c in range(CORES)] + [(0, 1)]

    def first_at(col, d, c):
        f, cc = lax.rem(first[col] + d, n_first[col]), lax.rem(core + c, CORES)
        return f * CORES + cc, dev_first(col, f, cc)

    def share_rows():
        for col in range(2):
            for v in range(2):
                z_buf[col, slot[col], pl.ds(v * batch, batch), :] = rows[v, pl.ds(0, batch), :]
            for o in first_offsets(col):
                for v in range(2):
                    remote(rows.at[v, pl.ds(0, batch)], z_buf.at[col, slot[col], pl.ds(v * batch, batch)],
                           z_send.at[col], z_recv.at[col], first_at(col, *o)[1]).start()

    share_rows()
    reduce_slice(0, 0)
    prob_sum = [softmax_terms(0)]
    reduce_slice(0, 1)
    share_scale(0, 0)
    prob_sum.append(softmax_terms(1))
    share_scale(0, 1)

    def iteration(it, carry):
        for v in range(2):
            next_pass(it, v)
        for v in range(2):
            reduce_slice(it + 1, v)
        for v in range(2):
            share_scale(it + 1, v)
        return carry

    lax.fori_loop(0, ITERS - 1, iteration, 0)
    last = ITERS - 1

    top = pl.ds(0, batch)

    def scaled(v, j):
        return mat[v, j, top, :] * ag_buf[last, v, lax.div(j, per), pl.ds(lax.rem(j, per), 1), :]

    def plan_sum(v):
        def step(t, acc):
            m = near(t)

            @pl.when(t > 0)
            def _():
                wait_scale(last, v, m)
            return acc + sum(mat[v, m * per + j, top, :] * ag_buf[last, v, m, pl.ds(j, 1), :] for j in range(per))
        acc = lax.fori_loop(0, members, step, jnp.zeros((batch, LANES), F32))
        return jnp.sum(acc, axis=1, keepdims=True)

    plan_inv = [1.0 / plan_sum(v) for v in range(2)]
    code_coef = [jnp.broadcast_to(plan_inv[v] * grad_coef, (batch, LANES)) for v in range(2)]
    prob_coef = [jnp.broadcast_to(grad_coef / prob_sum[v], (batch, LANES)) for v in range(2)]
    spread = width // LANES

    def g_start(col, h, m, device):
        block = (col * group[col] + m) * HALVES + h
        remote(grads.at[block], g_buf.at[col, h, slot[col]], g_send.at[col, h], g_recv.at[col, h], device).start()

    order = [(h, col) for h in range(HALVES) for col in range(2)]
    for h, col in order:
        def exchange_member(k):
            f = lax.rem(first[col] + near_offset(lax.div(k, 2)) + n_first[col], n_first[col])
            return f, lax.rem(core + lax.rem(k, 2), CORES)

        def make_block(t, carry, h=h, col=col, exchange_member=exchange_member):
            f, cc = exchange_member(group[col] - 1 - t)
            m = f * CORES + cc
            block = (col * group[col] + m) * HALVES + h
            for i in range(spread):
                j = block * spread + i
                lanes = pl.ds(pl.multiple_of(j * LANES, LANES), LANES)
                plans = [scaled(v, j) * code_coef[v] for v in range(2)]
                for v in range(2):
                    g = codes_refs[v][:, lanes] * prob_coef[v] - plans[1 - v]
                    grads[block, pl.ds(v * batch, batch), pl.ds(i * LANES, LANES)] = g.astype(BF16)

            @pl.when(t > 0)
            def _():
                f, cc = exchange_member(group[col] - t)
                g_start(col, h, f * CORES + cc, dev_first(col, f, cc))
            return carry

        lax.fori_loop(0, group[col], make_block, 0)
        g_buf[col, h, slot[col]] = grads[(col * group[col] + slot[col]) * HALVES + h]

    lse = [jnp.log(prob_sum[v]) for v in range(2)]

    def finish_chunk(t, carry):
        loss, dz = carry
        scores = [dot_nt(rows[v, top, :], cols[chunk_cols(t), :]) for v in range(2)]
        for i in range(spread):
            j = t * spread + i
            lanes = pl.ds(pl.multiple_of(j * LANES, LANES), LANES)
            for v in range(2):
                codes = scaled(v, j) * plan_inv[v]
                codes_refs[v][:, lanes] = codes
                other = scores[1 - v][:, i * LANES:(i + 1) * LANES]
                loss = loss + codes * (other * (1.0 / TEMPERATURE) - lse[1 - v])
        dz = dz + jnp.dot(grads[t], cols[chunk_cols(t), :], preferred_element_type=F32)
        return loss, dz

    def finish(t, carry):
        return finish_chunk(t * 2 + 1, finish_chunk(t * 2, carry))

    loss, dz = lax.fori_loop(0, chunks // 2, finish, (jnp.zeros((batch, LANES), F32), jnp.zeros((2 * batch, cols.shape[1]), F32)))
    dz_one[...] = dz[:batch]
    dz_two[...] = dz[batch:]
    loss_buf[0, slot[0]] = jnp.sum(loss, axis=0, keepdims=True)
    for o in first_offsets(0):
        remote(loss_buf.at[0, slot[0]], loss_buf.at[0, slot[0]], l_send.at[0], l_recv.at[0], first_at(0, *o)[1]).start()

    block_rows = [width // n_second[col] for col in range(2)]
    unit = block_rows[0] // nz

    def address(col, h, f, cc, s, zi):
        half_count = total.shape[0] // 2
        return col * half_count + ((f * CORES + cc) * HALVES + h) * width + s * block_rows[col] + zi * unit

    def rows_of(addr, n):
        return pl.ds(pl.multiple_of(addr, 8), n)

    def stage_g(h, col):
        wait_bytes(g_buf.at[col, h, pl.ds(0, group[col] - 1)], g_recv.at[col, h])
        if h == 0:
            wait_bytes(z_buf.at[col, pl.ds(0, group[col] - 1)], z_recv.at[col])
        k = group[col] * z_buf.shape[2]
        g = g_buf[col, h].reshape(k, width)
        zs = z_buf[col].reshape(k, z_buf.shape[3])
        part_buf[col, h] = lax.dot_general(g, zs, (((0,), (0,)), ((), ())), preferred_element_type=F32)
        for d in far_first(n_second[col]):
            s = lax.rem(second[col] + d, n_second[col])
            remote(part_buf.at[col, h, rows_of(s * block_rows[col], block_rows[col])], y_buf.at[col, h, second[col]],
                   p_send.at[col, h], p_recv.at[col, h], dev_second(col, s)).start()

    def stage_y(h, col):
        wait_bytes(y_buf.at[col, h, pl.ds(0, n_second[col] - 1)], p_recv.at[col, h])
        y_buf[col, h, second[col]] = part_buf[col, h, rows_of(second[col] * block_rows[col], block_rows[col])]
        yz_buf[col, h, 0] = jnp.sum(y_buf[col, h], axis=0)
        for d in far_first(nz):
            z2 = lax.rem(z + d, nz)
            remote(yz_buf.at[col, h, 0, rows_of(z2 * unit, unit)], sums.at[col, h, z],
                   s_send.at[col, h], s_recv.at[col, h], dev(x, y, z2, core)).start()

    def stage_z(h, col):
        wait_bytes(sums.at[col, h, pl.ds(0, nz - 1)], s_recv.at[col, h])
        sums[col, h, z] = yz_buf[col, h, 0, rows_of(z * unit, unit)]
        own = rows_of(address(col, h, first[col], core, second[col], z), unit)
        total[own, :] = jnp.sum(sums[col, h], axis=0)
        for d in far_first(nz):
            z2 = lax.rem(z + d, nz)
            remote(total.at[own], total.at[own], az_send.at[col, h], az_recv.at[col, h], dev(x, y, z2, core)).start()

    def stage_az(h, col):
        block = rows_of(address(col, h, first[col], core, second[col], 0), block_rows[col])
        wait_bytes(total.at[pl.ds(0, (nz - 1) * unit)], az_recv.at[col, h])
        for d in far_first(n_second[col]):
            s = lax.rem(second[col] + d, n_second[col])
            remote(total.at[block], total.at[block], ay_send.at[col, h], ay_recv.at[col, h], dev_second(col, s)).start()

    def pair_start(h, col, k, part):
        remote(total.at[part], total.at[part], pair_send.at[col, h, k], pair_recv.at[col, h, k],
               dev(x, y, z, 1 - core)).start()

    def stage_ay(h, col):
        n1 = n_first[col]
        wait_bytes(total.at[pl.ds(0, (n_second[col] - 1) * block_rows[col])], ay_recv.at[col, h])
        whole = rows_of(address(col, h, first[col], core, 0, 0), width)
        for d, step in enumerate((1, n1 - 1)):
            f = lax.rem(first[col] + step, n1)
            remote(total.at[whole], total.at[whole], ax_send.at[col, h, d], ax_recv.at[col, h, d],
                   dev_first(col, f, core)).start()
        pair_start(h, col, 0, whole)

    def stage_ax(h, col):
        n1 = n_first[col]
        for d, step in enumerate((1, n1 - 1)):
            src = lax.rem(first[col] + n1 - step, n1)
            nxt = lax.rem(first[col] + step, n1)
            whole = rows_of(address(col, h, src, core, 0, 0), width)
            wait_bytes(total.at[whole], ax_recv.at[col, h, d])
            part = rows_of(address(col, h, src, core, 0, 0) + d * (width // 2), width // 2)
            remote(total.at[part], total.at[part], af_send.at[col, h, d], af_recv.at[col, h, d],
                   dev_first(col, nxt, core)).start()
            pair_start(h, col, 1 + d, whole)

    def stage_af(h, col):
        n1 = n_first[col]
        src = lax.rem(first[col] + n1 // 2, n1)
        for d in range(2):
            part = rows_of(address(col, h, src, core, 0, 0) + d * (width // 2), width // 2)
            wait_bytes(total.at[part], af_recv.at[col, h, d])
            pair_start(h, col, 3 + d, part)

    def loss_stage(k):
        if k == 0:
            wait_bytes(loss_buf.at[0, pl.ds(0, group[0] - 1)], l_recv.at[0])
            loss_buf[1, y] = jnp.sum(loss_buf[0, pl.ds(0, group[0])], axis=0)
            for d in range(1, ny):
                remote(loss_buf.at[1, y], loss_buf.at[1, y], l_send.at[1], l_recv.at[1],
                       dev(x, lax.rem(y + d, ny), z, core)).start()
        elif k == 1:
            wait_bytes(loss_buf.at[1, pl.ds(0, ny - 1)], l_recv.at[1])
            loss_buf[2, z] = jnp.sum(loss_buf[1, pl.ds(0, ny)], axis=0)
            for d in range(1, nz):
                remote(loss_buf.at[2, z], loss_buf.at[2, z], l_send.at[2], l_recv.at[2],
                       dev(x, y, lax.rem(z + d, nz), core)).start()
        else:
            wait_bytes(loss_buf.at[2, pl.ds(0, nz - 1)], l_recv.at[2])
            terms = jnp.sum(loss_buf[2, pl.ds(0, nz)], axis=0)
            loss_out[...] = jnp.sum(terms, axis=1, keepdims=True) * loss_coef

    stages = [(stage_g, 0), (stage_y, 5), (stage_z, 10), (stage_az, 15), (stage_ay, 20), (stage_ax, 26), (stage_af, 30)]
    steps = sorted((at + 6 * h, k, h, col) for k, (_, at) in enumerate(stages) for h, col in order)
    for _, k, h, col in steps:
        stages[k][0](h, col)
        if (h, col) == (1, 1) and k < 3:
            loss_stage(k)

    for h, col in order:
        n1 = n_first[col]
        for k, src, off, n in (
            (0, first[col], 0, width),
            (1, lax.rem(first[col] + n1 - 1, n1), 0, width),
            (2, lax.rem(first[col] + 1, n1), 0, width),
            (3, lax.rem(first[col] + n1 // 2, n1), 0, width // 2),
            (4, lax.rem(first[col] + n1 // 2, n1), width // 2, width // 2),
        ):
            part = rows_of(address(col, h, src, 1 - core, 0, 0) + off, n)
            wait_bytes(total.at[part], pair_recv.at[col, h, k])
            wait_bytes(total.at[part], pair_send.at[col, h, k])

    def drain(it, carry):
        for v in range(2):
            wait_bytes(rs_buf.at[it, v, pl.ds(0, members - 1)], rs_send.at[it, v])
            wait_bytes(ex_buf.at[it, v, pl.ds(0, plane - 1)], ex_send.at[it, v])
            wait_bytes(rs_buf.at[it, v, pl.ds(0, members - 1)], ag_send.at[it, v])
        return carry

    lax.fori_loop(0, ITERS, drain, 0)
    for col in range(2):
        wait_bytes(z_buf.at[col, pl.ds(0, group[col] - 1)], z_send.at[col])
        for h in range(HALVES):
            wait_bytes(g_buf.at[col, h, pl.ds(0, group[col] - 1)], g_send.at[col, h])
            wait_bytes(y_buf.at[col, h, pl.ds(0, n_second[col] - 1)], p_send.at[col, h])
            wait_bytes(sums.at[col, h, pl.ds(0, nz - 1)], s_send.at[col, h])
            wait_bytes(total.at[pl.ds(0, (nz - 1) * unit)], az_send.at[col, h])
            wait_bytes(total.at[pl.ds(0, (n_second[col] - 1) * block_rows[col])], ay_send.at[col, h])
            for d in range(2):
                wait_bytes(total.at[pl.ds(0, width)], ax_send.at[col, h, d])
                wait_bytes(total.at[pl.ds(0, width // 2)], af_send.at[col, h, d])
    wait_bytes(loss_buf.at[0, pl.ds(0, group[0] - 1)], l_send.at[0])
    wait_bytes(loss_buf.at[1, pl.ds(0, ny - 1)], l_send.at[1])
    wait_bytes(loss_buf.at[2, pl.ds(0, nz - 1)], l_send.at[2])


def fused_step(nz, ny, nx, z_one, z_two, q_one, q_two, protos):
    batch, dim = z_one.shape
    n_rows = batch + q_one.shape[0]
    count = protos.shape[0]
    tiles = count // LANES
    members = nz * CORES
    plane = nx * ny
    devices = plane * members
    small = (tiles // members, LANES)
    group = nx * CORES
    chunks = 2 * HALVES * group
    width = count // chunks
    any_spec = pl.BlockSpec(memory_space=pl.ANY)
    vmem = pl.BlockSpec(memory_space=pltpu.VMEM)
    dma = pltpu.SemaphoreType.DMA
    two = dma((2, HALVES))
    out_bytes = 4 * (2 * batch * count + 2 * batch * dim + count * dim)
    return pl.pallas_call(
        functools.partial(
            step_kernel, nz, ny, nx, float(devices * n_rows), float(count),
            1.0 / (2 * devices * batch * TEMPERATURE), -1.0 / (2 * devices * batch)),
        out_shape=(
            pltpu.VMEM((batch, count), F32),
            pltpu.VMEM((batch, count), F32),
            pltpu.VMEM((1, 1), F32),
            pltpu.VMEM((batch, dim), F32),
            pltpu.VMEM((batch, dim), F32),
            pltpu.VMEM((count, dim), F32),
        ),
        in_specs=[any_spec] * 5,
        out_specs=(vmem,) * 6,
        scratch_shapes=[
            pltpu.VMEM((2, n_rows, dim), BF16),
            pltpu.VMEM((count, dim), BF16),
            pltpu.VMEM((2, tiles, n_rows, LANES), F32),
            pltpu.VMEM((n_rows, LANES), F32),
            pltpu.VMEM((n_rows, LANES), F32),
            pltpu.VMEM((ITERS, 2, members) + small, F32),
            pltpu.VMEM((ITERS, 2, members) + small, F32),
            pltpu.VMEM((ITERS, 2, plane) + small, F32),
            pltpu.VMEM((ITERS, 2, members) + small, F32),
            pltpu.VMEM((chunks, 2 * batch, width), BF16),
            pltpu.VMEM((2, HALVES, group, 2 * batch, width), BF16),
            pltpu.VMEM((2, group, 2 * batch, dim), BF16),
            pltpu.VMEM((2, HALVES, width, dim), F32),
            pltpu.VMEM((2, HALVES, ny, width // ny, dim), F32),
            pltpu.VMEM((2, HALVES, 1, width // ny, dim), F32),
            pltpu.VMEM((2, HALVES, nz, width // ny // nz, dim), F32),
            pltpu.VMEM((3, max(group, nz), 1, LANES), F32),
            dma((2, 2)),
            dma((members,)),
            dma((ITERS, 2)), dma((ITERS, 2)), dma((ITERS, 2)), dma((ITERS, 2)), dma((ITERS, 2)),
            dma((ITERS, 2, members)),
            dma((2,)), dma((2,)),
            two, two, two, two, two, two, two, two, two, two,
            dma((2, HALVES, 2)), dma((2, HALVES, 2)), dma((2, HALVES, 2)), dma((2, HALVES, 2)),
            dma((2, HALVES, 5)), dma((2, HALVES, 5)),
            dma((3,)), dma((3,)),
        ],
        compiler_params=pltpu.CompilerParams(
            collective_id=0, has_side_effects=True, vmem_limit_bytes=VMEM_TOTAL - out_bytes - 2 ** 16),
        name="step",
    )(z_one, z_two, q_one, q_two, protos)


def flush(arrays, piece=2 ** 20):
    n = len(arrays)
    cuts = []
    for i, a in enumerate(arrays):
        parts = max(1, 4 * a.size // piece)
        cuts += [(i, k * (a.shape[0] // parts), a.shape[0] // parts) for k in range(parts)]

    def kernel(*refs):
        sem = refs[-1]
        copies = [
            pltpu.make_async_copy(refs[i].at[pl.ds(at, count)], refs[n + i].at[pl.ds(at, count)], sem.at[k])
            for k, (i, at, count) in enumerate(cuts)]
        for c in copies:
            c.start()
        for c in copies:
            c.wait()

    return pl.pallas_call(
        kernel,
        out_shape=tuple(jax.ShapeDtypeStruct(a.shape, a.dtype) for a in arrays),
        in_specs=[pl.BlockSpec(memory_space=pltpu.VMEM)] * n,
        out_specs=(pl.BlockSpec(memory_space=pltpu.HBM),) * n,
        scratch_shapes=[pltpu.SemaphoreType.DMA((len(cuts),))],
        compiler_params=pltpu.CompilerParams(vmem_limit_bytes=2 ** 20),
        name="flush",
    )(*(pltpu.with_memory_space_constraint(a, pltpu.VMEM) for a in arrays))


def solution(mesh, nz=CHIPS_Z, nx=CHIPS_X):
    ny = mesh.shape["data"] // (nz * nx * CORES)

    def local_step(z_one, z_two, protos, queue_one, queue_two):
        outs = fused_step(nz, ny, nx, z_one, z_two, queue_one, queue_two, protos)
        codes_one, codes_two, loss, dz_one, dz_two, grad_protos = flush(outs)
        return codes_one, codes_two, loss.reshape(()), dz_one, dz_two, grad_protos

    row_spec = P("data", None)
    full_spec = P(None, None)
    return jax.shard_map(
        local_step,
        mesh=mesh,
        in_specs=(row_spec, row_spec, full_spec, row_spec, row_spec),
        out_specs=(row_spec, row_spec, P(), row_spec, row_spec, full_spec),
        check_vma=False,
    )
```
